128 devices in a mesh: patch: 64 (over y, x_hi, z, core), band: 2 (over x_lo).
Axes of the slice: x: 4 (x_hi: 2, x_lo: 2; x = x_hi * 2 + x_lo), y: 4, z: 4, core: 2. Of those that a mesh axis runs over, the one named last changes fastest.
Arguments:
- latents: float32 [40960, 512], P('patch', 'band'), may hold values from -6 to 6
- edge_latents: float32 [327680, 512], P(('patch', 'band')), may hold values from -6 to 6
- edge_sender: int32 [327680], P(('patch', 'band')), may hold values from 0 to 1343, as said below
- edge_receiver: int32 [327680], P(('patch', 'band')), may hold values from 0 to 319
- block_counts: int32 [2560], P(('patch', 'band')), may hold values from 16 to 128, as said below
- send_rows: int32 [128, 128, 8], P(('patch', 'band')), may hold values from 0 to 319
- edge_first_weight: bfloat16 [2, 1536, 512], replicated, may hold values from -0.15625 to 0.15625
- edge_first_bias: float32 [2, 512], replicated, may hold values from -3 to 3
- edge_second_weight: bfloat16 [2, 512, 512], replicated
- edge_gain: float32 [2, 512], replicated, may hold values from 0.1 to 1.9
- edge_offset: float32 [2, 512], replicated, may hold values from -3 to 3
- node_first_weight: bfloat16 [2, 1024, 512], replicated, may hold values from -0.1875 to 0.1875
- node_first_bias: float32 [2, 512], replicated, may hold values from -3 to 3
- node_second_weight: bfloat16 [2, 512, 512], replicated
- node_gain: float32 [2, 512], replicated, may hold values from 0.1 to 1.9
- node_offset: float32 [2, 512], replicated, may hold values from -3 to 3
Outputs:
- new_nodes: float32 [40960, 512], P(('patch', 'band'))
- new_edges: float32 [327680, 512], P(('patch', 'band'))
The draws below stay inside these ranges and needn't reach their ends.
Inputs may be any that keep to these rules, and one draw needn't show every extreme that they name: `edge_sender`: an entry below 320 names a node row of the edge's own device; an entry k above names slot (k - 320) % 8 of the rows that device (k - 320) // 8 sends to the edge's device. `block_counts`: the used slots of a block are its first ones; every device has a full block. send_rows[d, q] lists node rows of device d, numbered within d, that device q receives from d.
All inputs are finite; a program needn't handle non-finite values.
Results may differ from the reference program's by a relative error of at most 0.0045.
Values may be sent and summed in bfloat16 or wider, within the bound.
A program may use at most 128 MiB of HBM per device.

```python
import math
import jax
import jax.numpy as jnp
from jax import lax

D = 512
HID = 512
NODE_DEV = 320
BLOCKS = 20
BLOCK = 128
SLOT = 8
LAYERS = 2
SHARDS = 128
NODES = 40960
EDGE_DEV = 2560
EDGES = 327680


def draw_edge_sender(key, part):
    subkeys = jax.random.split(jax.random.fold_in(key, 5), 6)
    shape_two = (SHARDS, EDGE_DEV)
    lower = SLOT // 2 + 1
    counts = lower + jax.random.randint(subkeys[0], (SHARDS, SHARDS), 0, 1 << 20) % (SLOT + 1 - lower)
    fullest = jax.random.randint(subkeys[1], (SHARDS, 1), 0, SHARDS)
    counts = jnp.where(jnp.arange(SHARDS)[None, :] == fullest, SLOT, counts)
    local_rows = jax.random.randint(subkeys[2], shape_two, 0, NODE_DEV)
    source_shard = jax.random.randint(subkeys[3], shape_two, 0, SHARDS)
    spread_bits = jax.random.randint(subkeys[4], shape_two, 0, 1 << 20)
    chosen = jnp.take_along_axis(counts, source_shard, axis=1)
    remote = NODE_DEV + source_shard * SLOT + spread_bits % chosen
    picker = jax.random.randint(subkeys[5], shape_two, 0, 2)
    return jnp.where(picker == 0, local_rows, remote).reshape(-1).astype(jnp.int32)


def draw_block_counts(key, part):
    subkeys = jax.random.split(jax.random.fold_in(key, 7), 3)
    floor_value = max(1, BLOCK // 8)
    device_low = jax.random.randint(subkeys[0], (SHARDS, 1), floor_value, BLOCK + 1)
    raw_bits = jax.random.randint(subkeys[1], (SHARDS, BLOCKS), 0, 1 << 20)
    counts = device_low + raw_bits % (BLOCK + 1 - device_low)
    full_block = jax.random.randint(subkeys[2], (SHARDS, 1), 0, BLOCKS)
    counts = jnp.where(jnp.arange(BLOCKS)[None, :] == full_block, BLOCK, counts)
    return counts.reshape(-1).astype(jnp.int32)


def scaled_weight(key, depth_count, fan_rows, fan_cols):
    subkeys = jax.random.split(key, 2)
    base = jax.random.normal(subkeys[0], (depth_count, fan_rows, fan_cols), jnp.float32)
    column_scale = jnp.exp(jax.random.uniform(subkeys[1], (depth_count, 1, fan_cols), jnp.float32, math.log(0.3), math.log(3.0)))
    return base * column_scale * fan_rows ** (-0.5)


def draw_edge_second_weight(key, part):
    return scaled_weight(jax.random.fold_in(key, 21), LAYERS, HID, D).astype(jnp.bfloat16)


def draw_node_second_weight(key, part):
    return scaled_weight(jax.random.fold_in(key, 23), LAYERS, HID, D).astype(jnp.bfloat16)


def with_ends(array, stream_key, low, top_value):
    longest = array.shape.index(max(array.shape))
    spots = []
    for shift in (0, 1):
        where = [jax.random.randint(jax.random.fold_in(stream_key, axis), (), 0, length) for axis, length in enumerate(array.shape)]
        where[longest] = (where[longest] + shift) % array.shape[longest]
        spots.append(tuple(where))
    return array.at[spots[0]].set(low).at[spots[1]].set(top_value)


def levels(own_key, shape, cuts, low, largest):
    loudness = 1.0
    for dim, parts in cuts:
        heights = jax.random.uniform(jax.random.fold_in(jax.random.fold_in(own_key, 6), dim), (parts,), jnp.float32, low / len(cuts), largest / len(cuts))
        loudness = loudness * jnp.repeat(jnp.exp(heights), shape[dim] // parts).reshape((-1,) + (1,) * (len(shape) - 1 - dim))
    return loudness


def gaussian(own_key, dims, scale, limit, cuts=(), kind=jnp.bfloat16):
    values = jax.random.normal(own_key, dims, jnp.float32) * scale
    if len(cuts) > 0:
        values = levels(own_key, dims, cuts, -0.22, 0.18) * values
    return jnp.clip(values, min=-limit, max=limit).astype(kind)


def setup_inputs(seed: int = 0) -> dict:
    arg_keys = jax.random.split(jax.random.key(seed), 17)
    latents = gaussian(arg_keys[0], (NODES, D), 1.0, 6.0, ((0, 64), (1, 2)), jnp.float32)
    edge_latents = gaussian(arg_keys[1], (EDGES, D), 1.0, 6.0, ((0, 128),), jnp.float32)
    edge_sender = draw_edge_sender(jax.random.fold_in(arg_keys[16], 71), 0)
    edge_receiver = with_ends(jax.random.randint(arg_keys[3], (EDGES,), 0, NODE_DEV), jax.random.fold_in(arg_keys[3], 1), 0, NODE_DEV - 1).astype(jnp.int32)
    block_counts = draw_block_counts(jax.random.fold_in(arg_keys[16], 71), 0)
    send_rows = with_ends(jax.random.randint(arg_keys[5], (SHARDS, SHARDS, SLOT), 0, NODE_DEV), jax.random.fold_in(arg_keys[5], 1), 0, NODE_DEV - 1).astype(jnp.int32)
    edge_first_weight = gaussian(arg_keys[6], (LAYERS, 3 * D, HID), (3 * D) ** -0.5, 0.15625)
    edge_first_bias = gaussian(arg_keys[7], (LAYERS, HID), 0.5, 3.0, (), jnp.float32)
    edge_second_weight = draw_edge_second_weight(jax.random.fold_in(arg_keys[16], 71), 0)
    edge_gain = jnp.clip(1.0 + 0.18 * jax.random.normal(arg_keys[9], (LAYERS, D), jnp.float32), 0.1, 1.9)
    edge_offset = gaussian(arg_keys[10], (LAYERS, D), 0.5, 3.0, (), jnp.float32)
    node_first_weight = gaussian(arg_keys[11], (LAYERS, 2 * D, HID), (2 * D) ** -0.5, 0.1875)
    node_first_bias = gaussian(arg_keys[12], (LAYERS, HID), 0.5, 3.0, (), jnp.float32)
    node_second_weight = draw_node_second_weight(jax.random.fold_in(arg_keys[16], 71), 0)
    node_gain = jnp.clip(1.0 + 0.18 * jax.random.normal(arg_keys[14], (LAYERS, D), jnp.float32), 0.1, 1.9)
    node_offset = gaussian(arg_keys[15], (LAYERS, D), 0.5, 3.0, (), jnp.float32)
    return {"latents": latents, "edge_latents": edge_latents, "edge_sender": edge_sender, "edge_receiver": edge_receiver, "block_counts": block_counts, "send_rows": send_rows, "edge_first_weight": edge_first_weight, "edge_first_bias": edge_first_bias, "edge_second_weight": edge_second_weight, "edge_gain": edge_gain, "edge_offset": edge_offset, "node_first_weight": node_first_weight, "node_first_bias": node_first_bias, "node_second_weight": node_second_weight, "node_gain": node_gain, "node_offset": node_offset}


epsilon = 1e-05

def layer_norm(values, norm_gain, norm_offset):
    centre = values - lax.optimization_barrier(jnp.mean(values, axis=-1, keepdims=True))
    spread = lax.optimization_barrier(jnp.mean(centre * centre, axis=-1, keepdims=True))
    return centre * lax.rsqrt(spread + epsilon) * norm_gain + norm_offset

def perceptron(pieces, first_weight, first_bias, second_weight, norm_gain, norm_offset):
    columns = pieces[0].shape[1]
    running = first_bias
    for position in range(len(pieces)):
        running = running + jnp.dot(pieces[position], first_weight[position * columns:(position + 1) * columns], preferred_element_type=jnp.float32)
    active = (running * jax.nn.sigmoid(running)).astype(jnp.bfloat16)
    result = jnp.dot(active, second_weight, preferred_element_type=jnp.float32)
    return layer_norm(result, norm_gain, norm_offset)

def reference(latents, edge_latents, edge_sender, edge_receiver, block_counts, send_rows, edge_first_weight, edge_first_bias, edge_second_weight, edge_gain, edge_offset, node_first_weight, node_first_bias, node_second_weight, node_gain, node_offset):
    shards = NODES // NODE_DEV
    slot_index = jnp.arange(EDGES, dtype=jnp.int32)
    owning = slot_index // EDGE_DEV
    beyond = edge_sender - NODE_DEV
    source_shard = jnp.clip(beyond // SLOT, 0, shards - 1).astype(jnp.int32)
    slot_pos = jnp.clip(beyond % SLOT, 0, SLOT - 1).astype(jnp.int32)
    remote = source_shard * NODE_DEV + send_rows[source_shard, owning, slot_pos]
    senders = jnp.where(edge_sender < NODE_DEV, owning * NODE_DEV + edge_sender, remote).astype(jnp.int32)
    receivers = (owning * NODE_DEV + edge_receiver).astype(jnp.int32)
    usable = slot_index % BLOCK < block_counts[slot_index // BLOCK]
    node_state = latents
    edge_state = edge_latents
    for layer_index in range(LAYERS):
        node_low = node_state.astype(jnp.bfloat16)

        def portion(operands):
            edge_part, send_part, recv_part = operands
            return perceptron((edge_part.astype(jnp.bfloat16), node_low[send_part], node_low[recv_part]), edge_first_weight[layer_index], edge_first_bias[layer_index], edge_second_weight[layer_index], edge_gain[layer_index], edge_offset[layer_index])
        update = lax.map(portion, (edge_state.reshape(shards, EDGE_DEV, D), senders.reshape(shards, EDGE_DEV), receivers.reshape(shards, EDGE_DEV)))
        update = update.reshape(EDGES, D)
        edge_state = edge_state + jnp.where(usable[:, None], update, jnp.zeros_like(update))
        edge_out_low = lax.optimization_barrier(edge_state.astype(jnp.bfloat16)).astype(jnp.float32)
        summed = jax.ops.segment_sum(jnp.where(usable[:, None], edge_out_low, jnp.zeros_like(edge_out_low)), receivers, num_segments=NODES)
        summed_low = summed.astype(jnp.bfloat16)
        node_state = node_state + perceptron((node_low, summed_low), node_first_weight[layer_index], node_first_bias[layer_index], node_second_weight[layer_index], node_gain[layer_index], node_offset[layer_index])
    return (node_state, edge_state)
```

```python
import functools

import jax
import jax.numpy as jnp
from jax import lax
from jax.experimental import pallas as pl
from jax.experimental.pallas import tpu as pltpu
from jax.sharding import PartitionSpec as P

MESH = pl.DeviceIdType.MESH
F32 = jnp.float32
BF16 = jnp.bfloat16
D = 512
HALF = 256
ROWS = 320
EDGE = 2560
BLK = 256
NBLK = EDGE // BLK
EPS = 1e-05


def dot(a, b):
    return jnp.dot(a, b, preferred_element_type=F32)


def swish(v):
    half = 0.5 * v
    return half + half * jnp.tanh(half)


def norm(v, gain, offset):
    centre = v - jnp.sum(v, axis=-1, keepdims=True) * (1.0 / D)
    spread = jnp.sum(centre * centre, axis=-1, keepdims=True) * (1.0 / D)
    return centre * lax.rsqrt(spread + EPS) * gain + offset


def column(row):
    return jnp.transpose(jnp.broadcast_to(row, (128, 128)))


def hot(match):
    return jnp.where(match, 1.0, 0.0).astype(BF16)


def lanes(base):
    return (lax.broadcasted_iota(jnp.int32, (128, 128), 1) + base).astype(F32)


def edge_finish(pre, state, usable, w2, gain, offset):
    hidden = swish(pre).astype(BF16)
    update = norm(dot(hidden, w2), gain, offset)
    return state + jnp.where(usable, update, 0.0)


def usable_rows(counts, block):
    row = lax.broadcasted_iota(jnp.int32, (128, 1), 0)
    return jnp.concatenate([row < counts[2 * block], row < counts[2 * block + 1]], axis=0)


def summing(rcv, counts, block):
    node = lax.broadcasted_iota(jnp.int32, (ROWS, 128), 0)
    lane = lax.broadcasted_iota(jnp.int32, (1, 128), 1)
    parts = []
    for j in range(2):
        i = 2 * block + j
        target = jnp.where(lane < counts[i], rcv[pl.ds(i, 1), :], -1)
        parts.append(hot(node == target))
    return jnp.concatenate(parts, axis=1)


def node_finish(pv, summed, v1, w2, gain, offset):
    hidden = swish(pv + dot(summed.astype(BF16), v1)).astype(BF16)
    return norm(dot(hidden, w2), gain, offset)


def place():
    p = lax.axis_index("patch")
    b = lax.axis_index("band")
    core = p % 2
    z = (p // 2) % 4
    x = ((p // 8) % 2) * 2 + b
    y = p // 16
    return p, b, core, x, y, z


def at(core, x, y, z):
    return ((y * 2 + x // 2) * 4 + z) * 2 + core, x % 2


def turn(k):
    return k + (k // 2) * (1 - 2 * (k % 2))


def first_kernel(
    latents,
    edges,
    snd,
    rcv,
    counts,
    lists,
    we1,
    eb1,
    we2,
    egain,
    eoff,
    wn1,
    nb1,
    wn2,
    ngain,
    noff,
    pre_out,
    edge_out,
    node_out,
    pv_out,
    table_out,
    lat,
    state,
    pre,
    hot_local,
    hot_halo,
    hot_sum,
    hot_send,
    w1,
    w2,
    v1,
    v2,
    band_out,
    band_in,
    node,
    low,
    table,
    stage,
    recv,
    total,
    lat_sem,
    edge_sem,
    w_sem,
    band_send,
    band_recv,
    halo_send,
    halo_recv,
    out_sem,
    greet,
):
    p, b, core, x, y, z = place()
    me = p * 2 + b
    barrier = pltpu.get_barrier_semaphore()
    plane = [(0, 0, dy, dz) for dy in range(4) for dz in range(4) if (dy, dz) != (0, 0)]
    line = [(dc, dx, 0, 0) for dc in range(2) for dx in range(4) if (dc, dx) != (0, 0)]

    def peer(dc, dx, dy, dz):
        return at((core + dc) % 2, (x + dx) % 4, (y + dy) % 4, (z + dz) % 4)

    for o in plane + line:
        pl.semaphore_signal(barrier, inc=1, device_id=peer(*o), device_id_type=MESH)
    lat_copy = pltpu.make_async_copy(latents, lat, lat_sem)
    lat_copy.start()
    w_copies = [
        pltpu.make_async_copy(we1, w1, w_sem.at[0]),
        pltpu.make_async_copy(wn1, v1, w_sem.at[1]),
        pltpu.make_async_copy(we2.at[0], w2, w_sem.at[2]),
        pltpu.make_async_copy(wn2.at[0], v2, w_sem.at[3]),
    ]
    w_copies[0].start()
    edge_copies = [
        pltpu.make_async_copy(edges.at[pl.ds(i * 512, 512)], state.at[pl.ds(i * 512, 512)], edge_sem.at[i])
        for i in range(EDGE // 512)
    ]
    for c in edge_copies:
        c.start()
    for c in w_copies[1:]:
        c.start()
    lat_copy.wait()
    band_out[...] = lat[pl.ds((1 - b) * ROWS, ROWS), :].astype(BF16)

    for c in range(8):
        block = jnp.concatenate(
            [jnp.broadcast_to(lists[:, q : q + 1], (8, 128)) for q in range(16 * c, 16 * c + 16)], axis=0
        ).astype(F32)
        for t in range(3):
            wide = 128 if t < 2 else 64
            hot_send[c, :, t * 128 : t * 128 + wide] = hot(block == lanes(t * 128))[:, :wide]

    pl.semaphore_wait(barrier, len(plane) + len(line))
    for o in line:
        pl.semaphore_signal(greet, inc=1, device_id=peer(*o), device_id_type=MESH)
    pl.semaphore_wait(greet, len(line))
    band_copy = pltpu.make_async_remote_copy(
        src_ref=band_out,
        dst_ref=band_in,
        send_sem=band_send,
        recv_sem=band_recv,
        device_id=(p, 1 - b),
        device_id_type=MESH,
    )
    band_copy.start()

    def hots(i, _):
        rows = pl.ds(pl.multiple_of(i * 128, 128), 128)
        s = column(snd[pl.ds(i, 1), :].astype(F32))
        r = column(rcv[pl.ds(i, 1), :].astype(F32)) + float(ROWS)
        lane = lax.broadcasted_iota(jnp.int32, (128, 128), 1)
        mixed = jnp.where(lane < 64, s, r)
        for t, source in enumerate((s, s, mixed, r, r)):
            hot_local[rows, t * 128 : t * 128 + 128] = hot(source == lanes(t * 128))
        for t in range(8):
            hot_halo[t // 2, rows, (t % 2) * 128 : (t % 2) * 128 + 128] = hot(s == lanes(ROWS + t * 128))
        return 0

    lax.fori_loop(0, EDGE // 128, hots, 0)

    def sums(i, _):
        hot_sum[i] = summing(rcv, counts, i)
        return 0

    lax.fori_loop(0, NBLK, sums, 0)
    w_copies[0].wait()
    for c in edge_copies:
        c.wait()

    def edge_part(layer):
        def body(i, _):
            rows = pl.ds(pl.multiple_of(i * BLK, BLK), BLK)
            pre[rows, :] = dot(state[rows, :].astype(BF16), w1[layer, :D, :]) + eb1[pl.ds(layer, 1), :]
            return 0

        lax.fori_loop(0, NBLK, body, 0)

    edge_part(0)
    band_copy.wait()
    own = lat[pl.ds(b * ROWS, ROWS), :]
    other = band_in[...].astype(F32)
    node[:, :HALF] = jnp.where(b == 0, own, other)
    node[:, HALF:] = jnp.where(b == 0, other, own)
    for c in w_copies[1:]:
        c.wait()

    def exchange(layer):
        low[...] = node[...].astype(BF16)
        table[:ROWS, :] = dot(low[...], w1[layer, D : 2 * D, :]).astype(BF16)

        def fill(c, _):
            rows = dot(hot_send[c], table[:ROWS, :]).astype(BF16)
            stage[layer, pl.ds(c * 16, 16)] = rows.reshape(16, 8, D)
            return 0

        lax.fori_loop(0, 8, fill, 0)
        recv[layer, me] = stage[layer, me]

        def send(k, _):
            px, bx = at((core + k) % 2, (x + k // 2) % 4, (y + turn(k // 32)) % 4, (z + k // 8) % 4)
            pltpu.make_async_remote_copy(
                src_ref=stage.at[layer, px * 2 + bx],
                dst_ref=recv.at[layer, me],
                send_sem=halo_send.at[layer],
                recv_sem=halo_recv.at[layer, k // 32],
                device_id=(px, bx),
                device_id_type=MESH,
            ).start()
            return 0

        lax.fori_loop(1, 128, send, 0)
        table[ROWS:, :] = dot(low[...], w1[layer, 2 * D :, :]).astype(BF16)
        pv_out[...] = dot(low[...], v1[layer, :D, :]) + nb1[pl.ds(layer, 1), :]

    def local_part():
        def body(i, _):
            rows = pl.ds(pl.multiple_of(i * BLK, BLK), BLK)
            pre[rows, :] += dot(hot_local[rows, :], table[...])
            return 0

        lax.fori_loop(0, NBLK, body, 0)

    def wait_chunk(layer, c):
        n = 31 if c == 0 else 32
        pltpu.make_async_copy(
            stage.at[layer, pl.ds(0, n)], recv.at[layer, pl.ds(0, n)], halo_recv.at[layer, c]
        ).wait()
        return (y - (0, 1, 3, 2)[c] + 4) % 4

    def chunk_rows(layer, source):
        return recv[layer, pl.ds(source * 32, 32)].reshape(256, D)

    def halo_part(layer, c):
        source = wait_chunk(layer, c)

        def body(i, _):
            rows = pl.ds(pl.multiple_of(i * BLK, BLK), BLK)
            pre[rows, :] += dot(hot_halo[source, rows, :], chunk_rows(layer, source))
            return 0

        lax.fori_loop(0, NBLK, body, 0)

    def wait_sends(layer):
        pltpu.make_async_copy(
            stage.at[layer, pl.ds(0, 127)], recv.at[layer, pl.ds(0, 127)], halo_send.at[layer]
        ).wait()

    exchange(0)
    local_part()
    for c in range(3):
        halo_part(0, c)
    source = wait_chunk(0, 3)
    total[...] = jnp.zeros_like(total)

    def finish(i, _):
        rows = pl.ds(pl.multiple_of(i * BLK, BLK), BLK)
        value = pre[rows, :] + dot(hot_halo[source, rows, :], chunk_rows(0, source))
        done = edge_finish(value, state[rows, :], usable_rows(counts, i), w2[...], egain[0:1, :], eoff[0:1, :])
        state[rows, :] = done
        total[...] += dot(hot_sum[i], done.astype(BF16))
        return 0

    lax.fori_loop(0, NBLK, finish, 0)
    edge_copy = pltpu.make_async_copy(state, edge_out, out_sem.at[0])
    edge_copy.start()
    node[...] += node_finish(pv_out[...], total[...], v1[0, D:, :], v2[...], ngain[0:1, :], noff[0:1, :])
    wait_sends(0)
    exchange(1)
    node_out[...] = node[...]
    edge_part(1)
    local_part()
    for c in range(3):
        halo_part(1, c)
    pre_copy = pltpu.make_async_copy(pre, pre_out, out_sem.at[1])
    pre_copy.start()
    source = wait_chunk(1, 3)
    table_out[...] = chunk_rows(1, source)
    wait_sends(1)
    edge_copy.wait()
    pre_copy.wait()


def second_kernel(
    pre, state, snd, rcv, counts, table, node, pv, we2, egain, eoff, wn1, wn2, ngain, noff, edge_out, node_out, total
):
    i = pl.program_id(0)
    y = lax.axis_index("patch") // 16
    base = ROWS + ((y - 2 + 4) % 4) * 256
    halves = []
    for j in range(2):
        s = column(snd[pl.ds(2 * i + j, 1), :].astype(F32))
        halves.append(jnp.concatenate([hot(s == lanes(base + t * 128)) for t in range(2)], axis=1))
    value = pre[...] + dot(jnp.concatenate(halves, axis=0), table[...])
    done = edge_finish(value, state[...], usable_rows(counts, i), we2[...], egain[1:2, :], eoff[1:2, :])
    edge_out[...] = done

    @pl.when(i == 0)
    def _():
        total[...] = jnp.zeros_like(total)

    total[...] += dot(summing(rcv, counts, i), done.astype(BF16))

    @pl.when(i == NBLK - 1)
    def _():
        node_out[...] = node[...] + node_finish(pv[...], total[...], wn1[...], wn2[...], ngain[1:2, :], noff[1:2, :])


VMEM = pl.BlockSpec(memory_space=pltpu.VMEM)
SMEM = pl.BlockSpec(memory_space=pltpu.SMEM)
ANY = pl.BlockSpec(memory_space=pl.ANY)


def shards(
    latents,
    edge_latents,
    edge_sender,
    edge_receiver,
    block_counts,
    send_rows,
    edge_first_weight,
    edge_first_bias,
    edge_second_weight,
    edge_gain,
    edge_offset,
    node_first_weight,
    node_first_bias,
    node_second_weight,
    node_gain,
    node_offset,
):
    snd = edge_sender.reshape(EDGE // 128, 128)
    rcv = edge_receiver.reshape(EDGE // 128, 128)
    lists = jnp.transpose(send_rows[0])
    shape = jax.ShapeDtypeStruct
    pre, state, node, pv, table = pl.pallas_call(
        first_kernel,
        out_shape=(
            shape((EDGE, D), F32),
            shape((EDGE, D), F32),
            shape((ROWS, D), F32),
            shape((ROWS, D), F32),
            shape((256, D), BF16),
        ),
        in_specs=[ANY, ANY, VMEM, VMEM, SMEM, VMEM, ANY, VMEM, ANY, VMEM, VMEM, ANY, VMEM, ANY, VMEM, VMEM],
        out_specs=(ANY, ANY, VMEM, VMEM, VMEM),
        scratch_shapes=[
            pltpu.VMEM((2 * ROWS, HALF), F32),
            pltpu.VMEM((EDGE, D), F32),
            pltpu.VMEM((EDGE, D), F32),
            pltpu.VMEM((EDGE, 2 * ROWS), BF16),
            pltpu.VMEM((4, EDGE, 256), BF16),
            pltpu.VMEM((NBLK, ROWS, BLK), BF16),
            pltpu.VMEM((8, 128, ROWS), BF16),
            pltpu.VMEM((2, 3 * D, D), BF16),
            pltpu.VMEM((D, D), BF16),
            pltpu.VMEM((2, 2 * D, D), BF16),
            pltpu.VMEM((D, D), BF16),
            pltpu.VMEM((ROWS, HALF), BF16),
            pltpu.VMEM((ROWS, HALF), BF16),
            pltpu.VMEM((ROWS, D), F32),
            pltpu.VMEM((ROWS, D), BF16),
            pltpu.VMEM((2 * ROWS, D), BF16),
            pltpu.VMEM((2, 128, 8, D), BF16),
            pltpu.VMEM((2, 128, 8, D), BF16),
            pltpu.VMEM((ROWS, D), F32),
            pltpu.SemaphoreType.DMA,
            pltpu.SemaphoreType.DMA((EDGE // 512,)),
            pltpu.SemaphoreType.DMA((4,)),
            pltpu.SemaphoreType.DMA,
            pltpu.SemaphoreType.DMA,
            pltpu.SemaphoreType.DMA((2,)),
            pltpu.SemaphoreType.DMA((2, 4)),
            pltpu.SemaphoreType.DMA((2,)),
            pltpu.SemaphoreType.REGULAR,
        ],
        compiler_params=pltpu.CompilerParams(
            collective_id=0, has_side_effects=True, vmem_limit_bytes=56 * 1024 * 1024
        ),
    )(
        latents,
        edge_latents,
        snd,
        rcv,
        block_counts,
        lists,
        edge_first_weight,
        edge_first_bias,
        edge_second_weight,
        edge_gain,
        edge_offset,
        node_first_weight,
        node_first_bias,
        node_second_weight,
        node_gain,
        node_offset,
    )

    def whole(*dims):
        return pl.BlockSpec(dims, lambda i: (0,) * len(dims))

    new_edges, new_nodes = pl.pallas_call(
        second_kernel,
        grid=(NBLK,),
        out_shape=(shape((EDGE, D), F32), shape((ROWS, D), F32)),
        in_specs=[
            pl.BlockSpec((BLK, D), lambda i: (i, 0)),
            pl.BlockSpec((BLK, D), lambda i: (i, 0)),
            whole(EDGE // 128, 128),
            whole(EDGE // 128, 128),
            SMEM,
            whole(256, D),
            whole(ROWS, D),
            whole(ROWS, D),
            pl.BlockSpec((None, D, D), lambda i: (1, 0, 0)),
            whole(2, D),
            whole(2, D),
            pl.BlockSpec((None, D, D), lambda i: (1, 1, 0)),
            pl.BlockSpec((None, D, D), lambda i: (1, 0, 0)),
            whole(2, D),
            whole(2, D),
        ],
        out_specs=(pl.BlockSpec((BLK, D), lambda i: (i, 0)), whole(ROWS, D)),
        scratch_shapes=[pltpu.VMEM((ROWS, D), F32)],
        compiler_params=pltpu.CompilerParams(vmem_limit_bytes=40 * 1024 * 1024),
    )(
        pre,
        state,
        snd,
        rcv,
        block_counts,
        table,
        node,
        pv,
        edge_second_weight,
        edge_gain,
        edge_offset,
        node_first_weight,
        node_second_weight,
        node_gain,
        node_offset,
    )
    return new_nodes, new_edges


def solution(mesh):
    split = P(("patch", "band"))
    return jax.shard_map(
        shards,
        mesh=mesh,
        in_specs=(
            P("patch", "band"),
            P(("patch", "band"), None),
            split,
            split,
            split,
            P(("patch", "band"), None, None),
        )
        + (P(),) * 10,
        out_specs=(P(("patch", "band"), None), P(("patch", "band"), None)),
        check_vma=False,
    )
```

```python
import functools

import jax
import jax.numpy as jnp
from jax import lax
from jax.experimental import pallas as pl
from jax.experimental.pallas import tpu as pltpu
from jax.sharding import PartitionSpec as P

MESH = pl.DeviceIdType.MESH
F32 = jnp.float32
BF16 = jnp.bfloat16
D = 512
HALF = 256
ROWS = 320
EDGE = 2560
BIG = 512
NBIG = EDGE // BIG
EPS = 1e-05


def dot(a, b):
    return jnp.dot(a, b, preferred_element_type=F32)


def swish(v):
    half = 0.5 * v
    return half + half * jnp.tanh(half)


def norm(v, gain, offset):
    centre = v - jnp.sum(v, axis=-1, keepdims=True) * (1.0 / D)
    spread = jnp.sum(centre * centre, axis=-1, keepdims=True) * (1.0 / D)
    return centre * lax.rsqrt(spread + EPS) * gain + offset


def column(row):
    return jnp.transpose(jnp.broadcast_to(row, (128, 128)))


def hot(match):
    return jnp.where(match, 1.0, 0.0).astype(BF16)


def lanes(base):
    return (lax.broadcasted_iota(jnp.int32, (128, 128), 1) + base).astype(F32)


def strip(i, size):
    return slice(i * size, (i + 1) * size)


def finish_edges(pre, state, hot_last, rows, counts, w2, gain, offset, hidden, low, done):
    for i in range(NBIG):
        r = strip(i, BIG)
        half = pre[r, :] + dot(hot_last[r, :], rows)
        hidden[r, :] = (half + half * jnp.tanh(half)).astype(BF16)
    row = lax.broadcasted_iota(jnp.int32, (128, 1), 0)
    for i in range(NBIG):
        r = strip(i, BIG)
        n = BIG // 128
        usable = jnp.concatenate([row < counts[i * n + j] for j in range(n)], axis=0)
        update = norm(dot(hidden[r, :], w2), gain, offset)
        value = state[r, :] + jnp.where(usable, update, 0.0)
        low[r, :] = value.astype(BF16)
        done(i, value)


def node_finish(pv, summed, v1, w2, gain, offset):
    hidden = swish(pv + dot(summed.astype(BF16), v1)).astype(BF16)
    return norm(dot(hidden, w2), gain, offset)


def place():
    p = lax.axis_index("patch")
    b = lax.axis_index("band")
    core = p % 2
    z = (p // 2) % 4
    x = ((p // 8) % 2) * 2 + b
    y = p // 16
    return p, b, core, x, y, z


def at(core, x, y, z):
    return ((y * 2 + x // 2) * 4 + z) * 2 + core, x % 2


def first_kernel(
    latents,
    edges,
    snd,
    rcv,
    counts,
    lists,
    we1,
    eb1,
    we2,
    egain,
    eoff,
    wn1,
    nb1,
    wn2,
    ngain,
    noff,
    pre,
    state,
    node,
    pv,
    last_rows,
    hot_last,
    hot_sum,
    w2_next,
    v1_next,
    v2_next,
    lat,
    hot_halo,
    hot_local,
    hot_send,
    w1,
    w2,
    v1,
    v2,
    band_out,
    band_in,
    low,
    hidden,
    edge_low,
    table,
    stage,
    recv,
    lat_sem,
    edge_sem,
    w_sem,
    band_send,
    band_recv,
    halo_send,
    halo_recv,
    greet,
):
    p, b, core, x, y, z = place()
    me = p * 2 + b
    barrier = pltpu.get_barrier_semaphore()
    plane = [(0, 0, dy, dz) for dy in range(4) for dz in range(4) if (dy, dz) != (0, 0)]
    line = [(dc, dx, 0, 0) for dc in range(2) for dx in range(4) if (dc, dx) != (0, 0)]

    def peer(dc, dx, dy, dz):
        return at((core + dc) % 2, (x + dx) % 4, (y + dy) % 4, (z + dz) % 4)

    lat_copy = pltpu.make_async_copy(latents, lat, lat_sem)
    lat_copy.start()
    for o in plane + line:
        pl.semaphore_signal(barrier, inc=1, device_id=peer(*o), device_id_type=MESH)

    for c in range(8):
        block = jnp.concatenate(
            [jnp.broadcast_to(lists[:, q : q + 1], (8, 128)) for q in range(16 * c, 16 * c + 16)], axis=0
        ).astype(F32)
        for t in range(3):
            wide = 128 if t < 2 else 64
            hot_send[strip(c, 128), t * 128 : t * 128 + wide] = hot(block == lanes(t * 128))[:, :wide]

    lat_copy.wait()
    edge_copies = [
        pltpu.make_async_copy(edges.at[pl.ds(i * BIG, BIG)], state.at[pl.ds(i * BIG, BIG)], edge_sem.at[i])
        for i in range(NBIG)
    ]
    w_copies = [
        pltpu.make_async_copy(we1, w1, w_sem.at[0]),
        pltpu.make_async_copy(wn1, v1, w_sem.at[1]),
        pltpu.make_async_copy(we2.at[0], w2, w_sem.at[2]),
        pltpu.make_async_copy(wn2.at[0], v2, w_sem.at[3]),
        pltpu.make_async_copy(we2.at[1], w2_next, w_sem.at[4]),
        pltpu.make_async_copy(wn1.at[1, pl.ds(D, D)], v1_next, w_sem.at[5]),
        pltpu.make_async_copy(wn2.at[1], v2_next, w_sem.at[6]),
    ]
    w_copies[0].start()
    for c in edge_copies:
        c.start()
    for c in w_copies[1:]:
        c.start()
    band_out[...] = lat[pl.ds((1 - b) * ROWS, ROWS), :].astype(BF16)

    pl.semaphore_wait(barrier, len(plane) + len(line))
    for o in line:
        pl.semaphore_signal(greet, inc=1, device_id=peer(*o), device_id_type=MESH)
    pl.semaphore_wait(greet, len(line))
    band_copy = pltpu.make_async_remote_copy(
        src_ref=band_out,
        dst_ref=band_in,
        send_sem=band_send,
        recv_sem=band_recv,
        device_id=(p, 1 - b),
        device_id_type=MESH,
    )
    band_copy.start()

    def hots(i, _):
        rows = pl.ds(pl.multiple_of(i * 128, 128), 128)
        s = column(snd[pl.ds(i, 1), :].astype(F32))
        r = column(rcv[pl.ds(i, 1), :].astype(F32)) + float(ROWS)
        lane = lax.broadcasted_iota(jnp.int32, (128, 128), 1)
        mixed = jnp.where(lane < 64, s, r)
        for t, source in enumerate((s, s, mixed, r, r)):
            hot_local[rows, t * 128 : t * 128 + 128] = hot(source == lanes(t * 128))
        for t in range(8):
            hot_halo[t // 2, rows, (t % 2) * 128 : (t % 2) * 128 + 128] = hot(s == lanes(ROWS + t * 128))
        target = jnp.where(lane[:1] < counts[i], rcv[pl.ds(i, 1), :], -1)
        hot_sum[:, rows] = hot(lax.broadcasted_iota(jnp.int32, (ROWS, 128), 0) == target)
        return 0

    lax.fori_loop(0, EDGE // 128, hots, 0)
    w_copies[0].wait()
    for i in range(NBIG):
        edge_copies[i].wait()
        r = strip(i, BIG)
        pre[r, :] = 0.5 * (dot(state[r, :].astype(BF16), w1[0, :D, :]) + eb1[0:1, :])

    band_copy.wait()
    own = lat[pl.ds(b * ROWS, ROWS), :]
    other = band_in[...].astype(F32)
    node[:, :HALF] = jnp.where(b == 0, own, other)
    node[:, HALF:] = jnp.where(b == 0, other, own)
    for c in w_copies[1:]:
        c.wait()

    ys = [(y + d) % 4 for d in range(4)]
    xs = [(x + d) % 4 for d in range(4)]

    def exchange(layer):
        low[...] = node[...].astype(BF16)
        table[:ROWS, :] = (0.5 * dot(low[...], w1[layer, D : 2 * D, :])).astype(BF16)
        for c in range(8):
            rows = dot(hot_send[strip(c, 128), :], table[:ROWS, :]).astype(BF16)
            stage[layer, c * 16 : c * 16 + 16] = rows.reshape(16, 8, D)
        recv[layer, me] = stage[layer, me]

        def send(k, px, bx):
            pltpu.make_async_remote_copy(
                src_ref=stage.at[layer, px * 2 + bx],
                dst_ref=recv.at[layer, me],
                send_sem=halo_send.at[layer],
                recv_sem=halo_recv.at[layer, k],
                device_id=(px, bx),
                device_id_type=MESH,
            ).start()

        for group in ((1, 3), (2,), (0,)):

            def some(m, _):
                near = ((z + m // 2) % 4) * 2 + (core + m % 2) % 2
                for dx in range(4):
                    for dy in group:
                        px = ys[dy] * 16 + (xs[dx] // 2) * 8 + near
                        if dx == 0 and dy == 0:
                            pl.when(m > 0)(functools.partial(send, dy, px, xs[dx] % 2))
                        else:
                            send(dy, px, xs[dx] % 2)
                return 0

            lax.fori_loop(0, 8, some, 0)
        table[ROWS:, :] = (0.5 * dot(low[...], w1[layer, 2 * D :, :])).astype(BF16)
        pv[...] = dot(low[...], v1[layer, :D, :]) + nb1[layer : layer + 1, :]

    def wait_plane(layer, dy):
        n = 31 if dy == 0 else 32
        pltpu.make_async_copy(
            stage.at[layer, pl.ds(0, n)], recv.at[layer, pl.ds(0, n)], halo_recv.at[layer, dy]
        ).wait()
        return (y + 4 - dy) % 4

    def plane_rows(layer, source):
        return recv[layer, pl.ds(source * 32, 32)].reshape(256, D)

    def halo_part(layer, dy):
        source = wait_plane(layer, dy)
        for i in range(NBIG):
            r = strip(i, BIG)
            pre[r, :] += dot(hot_halo[source, r, :], plane_rows(layer, source))

    def wait_sends(layer):
        pltpu.make_async_copy(
            stage.at[layer, pl.ds(0, 127)], recv.at[layer, pl.ds(0, 127)], halo_send.at[layer]
        ).wait()

    exchange(0)
    for i in range(NBIG):
        r = strip(i, BIG)
        pre[r, :] += dot(hot_local[r, :], table[...])
    for dy in (1, 3, 2):
        halo_part(0, dy)
    source = wait_plane(0, 0)

    def keep(i, value):
        state[strip(i, BIG), :] = value

    finish_edges(
        pre,
        state,
        hot_halo.at[source],
        plane_rows(0, source),
        counts,
        w2[...],
        egain[0:1, :],
        eoff[0:1, :],
        hidden,
        edge_low,
        keep,
    )
    total = dot(hot_sum[...], edge_low[...])
    node[...] += node_finish(pv[...], total, v1[0, D:, :], v2[...], ngain[0:1, :], noff[0:1, :])
    exchange(1)
    for i in range(NBIG):
        r = strip(i, BIG)
        pre[r, :] = 0.5 * (dot(edge_low[r, :], w1[1, :D, :]) + eb1[1:2, :]) + dot(hot_local[r, :], table[...])
    for dy in (1, 3, 2):
        halo_part(1, dy)
    wait_sends(0)
    hot_last[...] = hot_halo[y]
    last_rows[...] = plane_rows(1, wait_plane(1, 0))
    wait_sends(1)


def second_kernel(
    pre,
    state,
    node,
    pv,
    last_rows,
    hot_last,
    hot_sum,
    w2,
    v1,
    v2,
    counts,
    egain,
    eoff,
    ngain,
    noff,
    edge_out,
    node_out,
    result,
    hidden,
    low,
    out_sem,
):
    copies = []

    def put(i, value):
        result[strip(i, BIG), :] = value
        copies.append(
            pltpu.make_async_copy(
                result.at[pl.ds(i * BIG, BIG)], edge_out.at[pl.ds(i * BIG, BIG)], out_sem.at[i]
            )
        )
        copies[-1].start()

    finish_edges(
        pre,
        state,
        hot_last,
        last_rows[...],
        counts,
        w2[...],
        egain[1:2, :],
        eoff[1:2, :],
        hidden,
        low,
        put,
    )
    total = dot(hot_sum[...], low[...])
    node_out[...] = node[...] + node_finish(pv[...], total, v1[...], v2[...], ngain[1:2, :], noff[1:2, :])
    for c in copies:
        c.wait()


VMEM = pl.BlockSpec(memory_space=pltpu.VMEM)
SMEM = pl.BlockSpec(memory_space=pltpu.SMEM)
ANY = pl.BlockSpec(memory_space=pl.ANY)
HBM = pl.BlockSpec(memory_space=pltpu.HBM)


def shards(
    latents,
    edge_latents,
    edge_sender,
    edge_receiver,
    block_counts,
    send_rows,
    edge_first_weight,
    edge_first_bias,
    edge_second_weight,
    edge_gain,
    edge_offset,
    node_first_weight,
    node_first_bias,
    node_second_weight,
    node_gain,
    node_offset,
):
    snd = edge_sender.reshape(EDGE // 128, 128)
    rcv = edge_receiver.reshape(EDGE // 128, 128)
    lists = jnp.transpose(send_rows[0])
    shape = jax.ShapeDtypeStruct
    held = pl.pallas_call(
        first_kernel,
        out_shape=(
            pltpu.VMEM((EDGE, D), F32),
            pltpu.VMEM((EDGE, D), F32),
            pltpu.VMEM((ROWS, D), F32),
            pltpu.VMEM((ROWS, D), F32),
            pltpu.VMEM((256, D), BF16),
            pltpu.VMEM((EDGE, 256), BF16),
            pltpu.VMEM((ROWS, EDGE), BF16),
            pltpu.VMEM((D, D), BF16),
            pltpu.VMEM((D, D), BF16),
            pltpu.VMEM((D, D), BF16),
        ),
        in_specs=[HBM, HBM, VMEM, VMEM, SMEM, VMEM, HBM, VMEM, HBM, VMEM, VMEM, HBM, VMEM, HBM, VMEM, VMEM],
        out_specs=(VMEM,) * 10,
        scratch_shapes=[
            pltpu.VMEM((2 * ROWS, HALF), F32),
            pltpu.VMEM((4, EDGE, 256), BF16),
            pltpu.VMEM((EDGE, 2 * ROWS), BF16),
            pltpu.VMEM((1024, ROWS), BF16),
            pltpu.VMEM((2, 3 * D, D), BF16),
            pltpu.VMEM((D, D), BF16),
            pltpu.VMEM((2, 2 * D, D), BF16),
            pltpu.VMEM((D, D), BF16),
            pltpu.VMEM((ROWS, HALF), BF16),
            pltpu.VMEM((ROWS, HALF), BF16),
            pltpu.VMEM((ROWS, D), BF16),
            pltpu.VMEM((EDGE, D), BF16),
            pltpu.VMEM((EDGE, D), BF16),
            pltpu.VMEM((2 * ROWS, D), BF16),
            pltpu.VMEM((2, 128, 8, D), BF16),
            pltpu.VMEM((2, 128, 8, D), BF16),
            pltpu.SemaphoreType.DMA,
            pltpu.SemaphoreType.DMA((NBIG,)),
            pltpu.SemaphoreType.DMA((7,)),
            pltpu.SemaphoreType.DMA,
            pltpu.SemaphoreType.DMA,
            pltpu.SemaphoreType.DMA((2,)),
            pltpu.SemaphoreType.DMA((2, 4)),
            pltpu.SemaphoreType.REGULAR,
        ],
        compiler_params=pltpu.CompilerParams(
            collective_id=0, has_side_effects=True, vmem_limit_bytes=47 * 1024 * 1024
        ),
    )(
        latents,
        edge_latents,
        snd,
        rcv,
        block_counts,
        lists,
        edge_first_weight,
        edge_first_bias,
        edge_second_weight,
        edge_gain,
        edge_offset,
        node_first_weight,
        node_first_bias,
        node_second_weight,
        node_gain,
        node_offset,
    )
    new_edges, new_nodes = pl.pallas_call(
        second_kernel,
        out_shape=(shape((EDGE, D), F32), shape((ROWS, D), F32)),
        in_specs=[VMEM] * 10 + [SMEM] + [VMEM] * 4,
        out_specs=(ANY, VMEM),
        scratch_shapes=[
            pltpu.VMEM((EDGE, D), F32),
            pltpu.VMEM((EDGE, D), BF16),
            pltpu.VMEM((EDGE, D), BF16),
            pltpu.SemaphoreType.DMA((NBIG,)),
        ],
        compiler_params=pltpu.CompilerParams(vmem_limit_bytes=24 * 1024 * 1024),
    )(
        *held,
        block_counts,
        edge_gain,
        edge_offset,
        node_gain,
        node_offset,
    )
    return new_nodes, new_edges


def solution(mesh):
    split = P(("patch", "band"))
    return jax.shard_map(
        shards,
        mesh=mesh,
        in_specs=(
            P("patch", "band"),
            P(("patch", "band"), None),
            split,
            split,
            split,
            P(("patch", "band"), None, None),
        )
        + (P(),) * 10,
        out_specs=(P(("patch", "band"), None), P(("patch", "band"), None)),
        check_vma=False,
    )
```

```python
import functools

import jax
import jax.numpy as jnp
from jax import lax
from jax.experimental import pallas as pl
from jax.experimental.pallas import tpu as pltpu
from jax.sharding import PartitionSpec as P

MESH = pl.DeviceIdType.MESH
F32 = jnp.float32
BF16 = jnp.bfloat16
D = 512
HALF = 256
ROWS = 320
EDGE = 2560
BIG = 512
NBIG = EDGE // BIG
EPS = 1e-05


def dot(a, b):
    return jnp.dot(a, b, preferred_element_type=F32)


def swish(v):
    half = 0.5 * v
    return half + half * jnp.tanh(half)


def norm(v, gain, offset):
    centre = v - jnp.sum(v, axis=-1, keepdims=True) * (1.0 / D)
    spread = jnp.sum(centre * centre, axis=-1, keepdims=True) * (1.0 / D)
    return centre * lax.rsqrt(spread + EPS) * gain + offset


def column(row):
    return jnp.transpose(jnp.broadcast_to(row, (128, 128)))


def hot(match):
    return jnp.where(match, 1.0, 0.0).astype(BF16)


def lanes(base):
    return (lax.broadcasted_iota(jnp.int32, (128, 128), 1) + base).astype(F32)


def strip(i, size):
    return slice(i * size, (i + 1) * size)


def finish_edges(pre, state, hot_last, rows, counts, w2, gain, offset, hidden, low, done):
    for i in range(NBIG):
        r = strip(i, BIG)
        half = pre[r, :] + dot(hot_last[r, :], rows)
        hidden[r, :] = (half + half * jnp.tanh(half)).astype(BF16)
    row = lax.broadcasted_iota(jnp.int32, (128, 1), 0)
    for i in range(NBIG):
        r = strip(i, BIG)
        n = BIG // 128
        usable = jnp.concatenate([row < counts[i * n + j] for j in range(n)], axis=0)
        update = norm(dot(hidden[r, :], w2), gain, offset)
        value = state[r, :] + jnp.where(usable, update, 0.0)
        low[r, :] = value.astype(BF16)
        done(i, value)


def node_finish(pv, summed, v1, w2, gain, offset):
    hidden = swish(pv + dot(summed.astype(BF16), v1)).astype(BF16)
    return norm(dot(hidden, w2), gain, offset)


def place():
    p = lax.axis_index("patch")
    b = lax.axis_index("band")
    core = p % 2
    z = (p // 2) % 4
    x = ((p // 8) % 2) * 2 + b
    y = p // 16
    return p, b, core, x, y, z


def at(core, x, y, z):
    return ((y * 2 + x // 2) * 4 + z) * 2 + core, x % 2


def first_kernel(
    latents,
    edges,
    snd_hbm,
    rcv_hbm,
    counts_hbm,
    lists_hbm,
    we1,
    eb1_hbm,
    we2,
    egain_hbm,
    eoff_hbm,
    wn1,
    nb1_hbm,
    wn2,
    ngain_hbm,
    noff_hbm,
    pre,
    state,
    node,
    pv,
    last_rows,
    hot_last,
    hot_sum,
    w2_next,
    v1_next,
    v2_next,
    snd,
    rcv,
    counts,
    lists,
    eb1,
    egain,
    eoff,
    nb1,
    ngain,
    noff,
    lat,
    hot_halo,
    hot_local,
    hot_send,
    w1,
    w2,
    v1,
    v2,
    band_out,
    band_in,
    low,
    hidden,
    edge_low,
    table,
    stage,
    recv,
    list_sem,
    lat_sem,
    edge_sem,
    w_sem,
    band_send,
    band_recv,
    halo_send,
    halo_recv,
    greet,
):
    p, b, core, x, y, z = place()
    me = p * 2 + b
    barrier = pltpu.get_barrier_semaphore()
    plane = [(0, 0, dy, dz) for dy in range(4) for dz in range(4) if (dy, dz) != (0, 0)]
    line = [(dc, dx, 0, 0) for dc in range(2) for dx in range(4) if (dc, dx) != (0, 0)]

    def peer(dc, dx, dy, dz):
        return at((core + dc) % 2, (x + dx) % 4, (y + dy) % 4, (z + dz) % 4)

    lat_copy = pltpu.make_async_copy(latents, lat, lat_sem)
    lat_copy.start()
    list_copy = pltpu.make_async_copy(lists_hbm, lists, list_sem)
    list_copy.start()
    for o in line + plane:
        pl.semaphore_signal(barrier, inc=1, device_id=peer(*o), device_id_type=MESH)
    w_copies = [
        pltpu.make_async_copy(source, target, w_sem.at[i])
        for i, (source, target) in enumerate(
            (
                (we1, w1),
                (snd_hbm, snd),
                (rcv_hbm, rcv),
                (counts_hbm, counts),
                (eb1_hbm, eb1),
                (wn1, v1),
                (nb1_hbm, nb1),
                (we2.at[0], w2),
                (egain_hbm, egain),
                (eoff_hbm, eoff),
                (wn2.at[0], v2),
                (ngain_hbm, ngain),
                (noff_hbm, noff),
                (we2.at[1], w2_next),
                (wn1.at[1, pl.ds(D, D)], v1_next),
                (wn2.at[1], v2_next),
            )
        )
    ]
    edge_copies = [
        pltpu.make_async_copy(edges.at[pl.ds(i * BIG, BIG)], state.at[pl.ds(i * BIG, BIG)], edge_sem.at[i])
        for i in range(NBIG)
    ]

    list_copy.wait()
    for c in range(8):
        block = jnp.concatenate(
            [jnp.broadcast_to(lists[:, q : q + 1], (8, 128)) for q in range(16 * c, 16 * c + 16)], axis=0
        ).astype(F32)
        for t in range(3):
            wide = 128 if t < 2 else 64
            hot_send[strip(c, 128), t * 128 : t * 128 + wide] = hot(block == lanes(t * 128))[:, :wide]

    lat_copy.wait()
    band_out[...] = lat[pl.ds((1 - b) * ROWS, ROWS), :].astype(BF16)
    for c in w_copies[:5] + edge_copies + w_copies[5:]:
        c.start()

    pl.semaphore_wait(barrier, len(plane) + len(line))
    for o in line:
        pl.semaphore_signal(greet, inc=1, device_id=peer(*o), device_id_type=MESH)
    band_copy = pltpu.make_async_remote_copy(
        src_ref=band_out,
        dst_ref=band_in,
        send_sem=band_send,
        recv_sem=band_recv,
        device_id=(p, 1 - b),
        device_id_type=MESH,
    )
    band_copy.start()
    w_copies[0].wait()
    band_copy.wait()
    own = lat[pl.ds(b * ROWS, ROWS), :]
    other = band_in[...].astype(F32)
    node[:, :HALF] = jnp.where(b == 0, own, other)
    node[:, HALF:] = jnp.where(b == 0, other, own)

    ys = [(y + d) % 4 for d in range(4)]
    xs = [(x + d) % 4 for d in range(4)]

    def exchange(layer):
        low[...] = node[...].astype(BF16)
        table[:ROWS, :] = (0.5 * dot(low[...], w1[layer, D : 2 * D, :])).astype(BF16)
        for c in range(8):
            rows = dot(hot_send[strip(c, 128), :], table[:ROWS, :]).astype(BF16)
            stage[layer, c * 16 : c * 16 + 16] = rows.reshape(16, 8, D)
        recv[layer, me] = stage[layer, me]
        if layer == 0:
            pl.semaphore_wait(greet, len(line))

        def send(k, px, bx):
            pltpu.make_async_remote_copy(
                src_ref=stage.at[layer, px * 2 + bx],
                dst_ref=recv.at[layer, me],
                send_sem=halo_send.at[layer],
                recv_sem=halo_recv.at[layer, k],
                device_id=(px, bx),
                device_id_type=MESH,
            ).start()

        for group in ((1, 3), (2,), (0,)):

            def some(m, _):
                near = ((z + m // 2) % 4) * 2 + (core + m % 2) % 2
                for dx in range(4):
                    for dy in group:
                        px = ys[dy] * 16 + (xs[dx] // 2) * 8 + near
                        if dx == 0 and dy == 0:
                            pl.when(m > 0)(functools.partial(send, dy, px, xs[dx] % 2))
                        else:
                            send(dy, px, xs[dx] % 2)
                return 0

            lax.fori_loop(0, 8, some, 0)

    def tables(layer):
        table[ROWS:, :] = (0.5 * dot(low[...], w1[layer, 2 * D :, :])).astype(BF16)
        pv[...] = dot(low[...], v1[layer, :D, :]) + nb1[layer : layer + 1, :]

    def wait_plane(layer, dy):
        n = 31 if dy == 0 else 32
        pltpu.make_async_copy(
            stage.at[layer, pl.ds(0, n)], recv.at[layer, pl.ds(0, n)], halo_recv.at[layer, dy]
        ).wait()
        return (y + 4 - dy) % 4

    def plane_rows(layer, source):
        return recv[layer, pl.ds(source * 32, 32)].reshape(256, D)

    def halo_part(layer, dy):
        source = wait_plane(layer, dy)
        for i in range(NBIG):
            r = strip(i, BIG)
            pre[r, :] += dot(hot_halo[source, r, :], plane_rows(layer, source))

    def wait_sends(layer):
        pltpu.make_async_copy(
            stage.at[layer, pl.ds(0, 127)], recv.at[layer, pl.ds(0, 127)], halo_send.at[layer]
        ).wait()

    exchange(0)
    for c in w_copies[1:5]:
        c.wait()

    def hots(i, _):
        rows = pl.ds(pl.multiple_of(i * 128, 128), 128)
        s = column(snd[pl.ds(i, 1), :].astype(F32))
        r = column(rcv[pl.ds(i, 1), :].astype(F32)) + float(ROWS)
        lane = lax.broadcasted_iota(jnp.int32, (128, 128), 1)
        mixed = jnp.where(lane < 64, s, r)
        for t, source in enumerate((s, s, mixed, r, r)):
            hot_local[rows, t * 128 : t * 128 + 128] = hot(source == lanes(t * 128))
        for t in range(8):
            hot_halo[t // 2, rows, (t % 2) * 128 : (t % 2) * 128 + 128] = hot(s == lanes(ROWS + t * 128))
        target = jnp.where(lane[:1] < counts[i], rcv[pl.ds(i, 1), :], -1)
        hot_sum[:, rows] = hot(lax.broadcasted_iota(jnp.int32, (ROWS, 128), 0) == target)
        return 0

    lax.fori_loop(0, EDGE // 128, hots, 0)
    for c in edge_copies + w_copies[5:]:
        c.wait()
    tables(0)
    for i in range(NBIG):
        r = strip(i, BIG)
        edge_part = 0.5 * (dot(state[r, :].astype(BF16), w1[0, :D, :]) + eb1[0:1, :])
        pre[r, :] = edge_part + dot(hot_local[r, :], table[...])
    for dy in (0, 1, 3):
        halo_part(0, dy)
    source = wait_plane(0, 2)

    def keep(i, value):
        state[strip(i, BIG), :] = value

    finish_edges(
        pre,
        state,
        hot_halo.at[source],
        plane_rows(0, source),
        counts,
        w2[...],
        egain[0:1, :],
        eoff[0:1, :],
        hidden,
        edge_low,
        keep,
    )
    total = dot(hot_sum[...], edge_low[...])
    node[...] += node_finish(pv[...], total, v1[0, D:, :], v2[...], ngain[0:1, :], noff[0:1, :])
    exchange(1)
    tables(1)
    for i in range(NBIG):
        r = strip(i, BIG)
        pre[r, :] = 0.5 * (dot(edge_low[r, :], w1[1, :D, :]) + eb1[1:2, :]) + dot(hot_local[r, :], table[...])
    for dy in (0, 1, 3):
        halo_part(1, dy)
    wait_sends(0)
    hot_last[...] = hot_halo[(y + 2) % 4]
    last_rows[...] = plane_rows(1, wait_plane(1, 2))
    wait_sends(1)


def second_kernel(
    pre,
    state,
    node,
    pv,
    last_rows,
    hot_last,
    hot_sum,
    w2,
    v1,
    v2,
    counts,
    egain,
    eoff,
    ngain,
    noff,
    edge_out,
    node_out,
    result,
    hidden,
    low,
    out_sem,
):
    copies = []

    def put(i, value):
        result[strip(i, BIG), :] = value
        copies.append(
            pltpu.make_async_copy(
                result.at[pl.ds(i * BIG, BIG)], edge_out.at[pl.ds(i * BIG, BIG)], out_sem.at[i]
            )
        )
        copies[-1].start()

    finish_edges(
        pre,
        state,
        hot_last,
        last_rows[...],
        counts,
        w2[...],
        egain[1:2, :],
        eoff[1:2, :],
        hidden,
        low,
        put,
    )
    total = dot(hot_sum[...], low[...])
    node_out[...] = node[...] + node_finish(pv[...], total, v1[...], v2[...], ngain[1:2, :], noff[1:2, :])
    for c in copies:
        c.wait()


VMEM = pl.BlockSpec(memory_space=pltpu.VMEM)
SMEM = pl.BlockSpec(memory_space=pltpu.SMEM)
ANY = pl.BlockSpec(memory_space=pl.ANY)
HBM = pl.BlockSpec(memory_space=pltpu.HBM)


def shards(
    latents,
    edge_latents,
    edge_sender,
    edge_receiver,
    block_counts,
    send_rows,
    edge_first_weight,
    edge_first_bias,
    edge_second_weight,
    edge_gain,
    edge_offset,
    node_first_weight,
    node_first_bias,
    node_second_weight,
    node_gain,
    node_offset,
):
    snd = edge_sender.reshape(EDGE // 128, 128)
    rcv = edge_receiver.reshape(EDGE // 128, 128)
    lists = jnp.transpose(send_rows[0])
    shape = jax.ShapeDtypeStruct
    held = pl.pallas_call(
        first_kernel,
        out_shape=(
            pltpu.VMEM((EDGE, D), F32),
            pltpu.VMEM((EDGE, D), F32),
            pltpu.VMEM((ROWS, D), F32),
            pltpu.VMEM((ROWS, D), F32),
            pltpu.VMEM((256, D), BF16),
            pltpu.VMEM((EDGE, 256), BF16),
            pltpu.VMEM((ROWS, EDGE), BF16),
            pltpu.VMEM((D, D), BF16),
            pltpu.VMEM((D, D), BF16),
            pltpu.VMEM((D, D), BF16),
        ),
        in_specs=[HBM] * 16,
        out_specs=(VMEM,) * 10,
        scratch_shapes=[
            pltpu.VMEM((EDGE // 128, 128), jnp.int32),
            pltpu.VMEM((EDGE // 128, 128), jnp.int32),
            pltpu.SMEM((EDGE // 128,), jnp.int32),
            pltpu.VMEM((8, 128), jnp.int32),
        ]
        + [pltpu.VMEM((2, D), F32)] * 6
        + [
            pltpu.VMEM((2 * ROWS, HALF), F32),
            pltpu.VMEM((4, EDGE, 256), BF16),
            pltpu.VMEM((EDGE, 2 * ROWS), BF16),
            pltpu.VMEM((1024, ROWS), BF16),
            pltpu.VMEM((2, 3 * D, D), BF16),
            pltpu.VMEM((D, D), BF16),
            pltpu.VMEM((2, 2 * D, D), BF16),
            pltpu.VMEM((D, D), BF16),
            pltpu.VMEM((ROWS, HALF), BF16),
            pltpu.VMEM((ROWS, HALF), BF16),
            pltpu.VMEM((ROWS, D), BF16),
            pltpu.VMEM((EDGE, D), BF16),
            pltpu.VMEM((EDGE, D), BF16),
            pltpu.VMEM((2 * ROWS, D), BF16),
            pltpu.VMEM((2, 128, 8, D), BF16),
            pltpu.VMEM((2, 128, 8, D), BF16),
            pltpu.SemaphoreType.DMA,
            pltpu.SemaphoreType.DMA,
            pltpu.SemaphoreType.DMA((NBIG,)),
            pltpu.SemaphoreType.DMA((16,)),
            pltpu.SemaphoreType.DMA,
            pltpu.SemaphoreType.DMA,
            pltpu.SemaphoreType.DMA((2,)),
            pltpu.SemaphoreType.DMA((2, 4)),
            pltpu.SemaphoreType.REGULAR,
        ],
        compiler_params=pltpu.CompilerParams(
            collective_id=0, has_side_effects=True, vmem_limit_bytes=47 * 1024 * 1024
        ),
    )(
        latents,
        edge_latents,
        snd,
        rcv,
        block_counts,
        lists,
        edge_first_weight,
        edge_first_bias,
        edge_second_weight,
        edge_gain,
        edge_offset,
        node_first_weight,
        node_first_bias,
        node_second_weight,
        node_gain,
        node_offset,
    )
    new_edges, new_nodes = pl.pallas_call(
        second_kernel,
        out_shape=(shape((EDGE, D), F32), shape((ROWS, D), F32)),
        in_specs=[VMEM] * 10 + [SMEM] + [VMEM] * 4,
        out_specs=(ANY, VMEM),
        scratch_shapes=[
            pltpu.VMEM((EDGE, D), F32),
            pltpu.VMEM((EDGE, D), BF16),
            pltpu.VMEM((EDGE, D), BF16),
            pltpu.SemaphoreType.DMA((NBIG,)),
        ],
        compiler_params=pltpu.CompilerParams(vmem_limit_bytes=24 * 1024 * 1024),
    )(
        *held,
        block_counts,
        edge_gain,
        edge_offset,
        node_gain,
        node_offset,
    )
    return new_nodes, new_edges


def solution(mesh):
    split = P(("patch", "band"))
    return jax.shard_map(
        shards,
        mesh=mesh,
        in_specs=(
            P("patch", "band"),
            P(("patch", "band"), None),
            split,
            split,
            split,
            P(("patch", "band"), None, None),
        )
        + (P(),) * 10,
        out_specs=(P(("patch", "band"), None), P(("patch", "band"), None)),
        check_vma=False,
    )
```

```python
import functools

import jax
import jax.numpy as jnp
from jax import lax
from jax.experimental import pallas as pl
from jax.experimental.pallas import tpu as pltpu
from jax.sharding import PartitionSpec as P

MESH = pl.DeviceIdType.MESH
F32 = jnp.float32
BF16 = jnp.bfloat16
D = 512
HALF = 256
ROWS = 320
EDGE = 2560
BIG = 512
NBIG = EDGE // BIG
EPS = 1e-05
ORDER = (1, 3, 2, 0)


def dot(a, b):
    return jnp.dot(a, b, preferred_element_type=F32)


def swish(v):
    half = 0.5 * v
    return half + half * jnp.tanh(half)


def norm(v, gain, offset):
    centre = v - jnp.sum(v, axis=-1, keepdims=True) * (1.0 / D)
    spread = jnp.sum(centre * centre, axis=-1, keepdims=True) * (1.0 / D)
    return centre * lax.rsqrt(spread + EPS) * gain + offset


def column(row):
    return jnp.transpose(jnp.broadcast_to(row, (128, 128)))


def hot(match):
    return jnp.where(match, 1.0, 0.0).astype(BF16)


def lanes(base):
    return (lax.broadcasted_iota(jnp.int32, (128, 128), 1) + base).astype(F32)


def strip(i, size):
    return slice(i * size, (i + 1) * size)


def finish_edges(pre, state, hot_last, rows, counts, w2, gain, offset, hidden, low, done):
    for i in range(NBIG):
        r = strip(i, BIG)
        half = pre[r, :] + dot(hot_last[r, :], rows)
        hidden[r, :] = (half + half * jnp.tanh(half)).astype(BF16)
    row = lax.broadcasted_iota(jnp.int32, (128, 1), 0)
    for i in range(NBIG):
        r = strip(i, BIG)
        n = BIG // 128
        usable = jnp.concatenate([row < counts[i * n + j] for j in range(n)], axis=0)
        update = norm(dot(hidden[r, :], w2), gain, offset)
        value = state[r, :] + jnp.where(usable, update, 0.0)
        low[r, :] = value.astype(BF16)
        done(i, value)


def node_finish(pv, summed, v1, w2, gain, offset):
    hidden = swish(pv + dot(summed.astype(BF16), v1)).astype(BF16)
    return norm(dot(hidden, w2), gain, offset)


def place():
    p = lax.axis_index("patch")
    b = lax.axis_index("band")
    core = p % 2
    z = (p // 2) % 4
    x = ((p // 8) % 2) * 2 + b
    y = p // 16
    return p, b, core, x, y, z


def at(core, x, y, z):
    return ((y * 2 + x // 2) * 4 + z) * 2 + core, x % 2


def first_kernel(
    latents,
    edges,
    snd_hbm,
    rcv_hbm,
    counts_hbm,
    lists_hbm,
    we1,
    eb1_hbm,
    we2,
    egain_hbm,
    eoff_hbm,
    wn1,
    nb1_hbm,
    wn2,
    ngain_hbm,
    noff_hbm,
    pre,
    state,
    node,
    pv,
    last_rows,
    hot_last,
    hot_sum,
    w2_next,
    v1_next,
    v2_next,
    snd,
    rcv,
    counts,
    lists,
    eb1,
    egain,
    eoff,
    nb1,
    ngain,
    noff,
    lat,
    hot_halo,
    hot_local,
    hot_send,
    w1,
    w2,
    v1,
    v2,
    band_out,
    band_in,
    low,
    hidden,
    edge_low,
    table,
    stage,
    recv,
    list_sem,
    lat_sem,
    edge_sem,
    w_sem,
    band_send,
    band_recv,
    halo_send,
    halo_recv,
    greet,
):
    p, b, core, x, y, z = place()
    me = p * 2 + b
    barrier = pltpu.get_barrier_semaphore()
    plane = [(0, 0, dy, dz) for dy in range(4) for dz in range(4) if (dy, dz) != (0, 0)]
    line = [(dc, dx, 0, 0) for dc in range(2) for dx in range(4) if (dc, dx) != (0, 0)]

    def peer(dc, dx, dy, dz):
        return at((core + dc) % 2, (x + dx) % 4, (y + dy) % 4, (z + dz) % 4)

    lat_copy = pltpu.make_async_copy(latents, lat, lat_sem)
    lat_copy.start()
    list_copy = pltpu.make_async_copy(lists_hbm, lists, list_sem)
    list_copy.start()
    for o in line + plane:
        pl.semaphore_signal(barrier, inc=1, device_id=peer(*o), device_id_type=MESH)
    w_copies = [
        pltpu.make_async_copy(source, target, w_sem.at[i])
        for i, (source, target) in enumerate(
            (
                (we1, w1),
                (snd_hbm, snd),
                (rcv_hbm, rcv),
                (counts_hbm, counts),
                (eb1_hbm, eb1),
                (wn1, v1),
                (nb1_hbm, nb1),
                (we2.at[0], w2),
                (egain_hbm, egain),
                (eoff_hbm, eoff),
                (wn2.at[0], v2),
                (ngain_hbm, ngain),
                (noff_hbm, noff),
                (we2.at[1], w2_next),
                (wn1.at[1, pl.ds(D, D)], v1_next),
                (wn2.at[1], v2_next),
            )
        )
    ]
    edge_copies = [
        pltpu.make_async_copy(edges.at[pl.ds(i * BIG, BIG)], state.at[pl.ds(i * BIG, BIG)], edge_sem.at[i])
        for i in range(NBIG)
    ]

    list_copy.wait()
    for c in range(8):
        block = jnp.concatenate(
            [jnp.broadcast_to(lists[:, q : q + 1], (8, 128)) for q in range(16 * c, 16 * c + 16)], axis=0
        ).astype(F32)
        for t in range(3):
            wide = 128 if t < 2 else 64
            hot_send[strip(c, 128), t * 128 : t * 128 + wide] = hot(block == lanes(t * 128))[:, :wide]

    lat_copy.wait()
    band_out[...] = lat[pl.ds((1 - b) * ROWS, ROWS), :].astype(BF16)
    for c in w_copies[:5] + edge_copies + w_copies[5:]:
        c.start()

    pl.semaphore_wait(barrier, len(plane) + len(line))
    for o in line:
        pl.semaphore_signal(greet, inc=1, device_id=peer(*o), device_id_type=MESH)
    band_copy = pltpu.make_async_remote_copy(
        src_ref=band_out,
        dst_ref=band_in,
        send_sem=band_send,
        recv_sem=band_recv,
        device_id=(p, 1 - b),
        device_id_type=MESH,
    )
    band_copy.start()
    w_copies[0].wait()
    band_copy.wait()
    own = lat[pl.ds(b * ROWS, ROWS), :]
    other = band_in[...].astype(F32)
    node[:, :HALF] = jnp.where(b == 0, own, other)
    node[:, HALF:] = jnp.where(b == 0, other, own)

    ys = [(y + d) % 4 for d in range(4)]
    xs = [(x + d) % 4 for d in range(4)]

    def exchange(layer):
        low[...] = node[...].astype(BF16)
        table[:ROWS, :] = (0.5 * dot(low[...], w1[layer, D : 2 * D, :])).astype(BF16)

        def fill(dy):
            rows = pl.ds(pl.multiple_of(ys[dy] * 256, 256), 256)
            chosen = dot(hot_send[rows, :], table[:ROWS, :]).astype(BF16)
            stage[layer, pl.ds(ys[dy] * 32, 32)] = chosen.reshape(32, 8, D)

        def send(k, px, bx):
            pltpu.make_async_remote_copy(
                src_ref=stage.at[layer, px * 2 + bx],
                dst_ref=recv.at[layer, me],
                send_sem=halo_send.at[layer],
                recv_sem=halo_recv.at[layer, k],
                device_id=(px, bx),
                device_id_type=MESH,
            ).start()

        def send_plane(dy):
            def some(m, _):
                near = ((z + m // 2) % 4) * 2 + (core + m % 2) % 2
                for dx in range(4):
                    px = ys[dy] * 16 + (xs[dx] // 2) * 8 + near
                    if dx == 0 and dy == 0:
                        pl.when(m > 0)(functools.partial(send, dy, px, xs[dx] % 2))
                    else:
                        send(dy, px, xs[dx] % 2)
                return 0

            lax.fori_loop(0, 8, some, 0)

        fill(ORDER[0])
        if layer == 0:
            pl.semaphore_wait(greet, len(line))
        for i in range(4):
            if i < 3:
                fill(ORDER[i + 1])
            send_plane(ORDER[i])
        recv[layer, me] = stage[layer, me]

    def tables(layer):
        table[ROWS:, :] = (0.5 * dot(low[...], w1[layer, 2 * D :, :])).astype(BF16)
        pv[...] = dot(low[...], v1[layer, :D, :]) + nb1[layer : layer + 1, :]

    def wait_plane(layer, dy):
        n = 31 if dy == 0 else 32
        pltpu.make_async_copy(
            stage.at[layer, pl.ds(0, n)], recv.at[layer, pl.ds(0, n)], halo_recv.at[layer, dy]
        ).wait()
        return (y + 4 - dy) % 4

    def plane_rows(layer, source):
        return recv[layer, pl.ds(source * 32, 32)].reshape(256, D)

    def halo_part(layer, dy):
        source = wait_plane(layer, dy)
        for i in range(NBIG):
            r = strip(i, BIG)
            pre[r, :] += dot(hot_halo[source, r, :], plane_rows(layer, source))

    def wait_sends(layer):
        pltpu.make_async_copy(
            stage.at[layer, pl.ds(0, 127)], recv.at[layer, pl.ds(0, 127)], halo_send.at[layer]
        ).wait()

    exchange(0)
    for c in w_copies[1:5]:
        c.wait()

    def hots(i, _):
        rows = pl.ds(pl.multiple_of(i * 128, 128), 128)
        s = column(snd[pl.ds(i, 1), :].astype(F32))
        r = column(rcv[pl.ds(i, 1), :].astype(F32)) + float(ROWS)
        lane = lax.broadcasted_iota(jnp.int32, (128, 128), 1)
        mixed = jnp.where(lane < 64, s, r)
        for t, source in enumerate((s, s, mixed, r, r)):
            hot_local[rows, t * 128 : t * 128 + 128] = hot(source == lanes(t * 128))
        for t in range(8):
            hot_halo[t // 2, rows, (t % 2) * 128 : (t % 2) * 128 + 128] = hot(s == lanes(ROWS + t * 128))
        target = jnp.where(lane[:1] < counts[i], rcv[pl.ds(i, 1), :], -1)
        hot_sum[:, rows] = hot(lax.broadcasted_iota(jnp.int32, (ROWS, 128), 0) == target)
        return 0

    lax.fori_loop(0, EDGE // 128, hots, 0)
    for c in edge_copies + w_copies[5:]:
        c.wait()
    tables(0)
    for i in range(NBIG):
        r = strip(i, BIG)
        edge_part = 0.5 * (dot(state[r, :].astype(BF16), w1[0, :D, :]) + eb1[0:1, :])
        pre[r, :] = edge_part + dot(hot_local[r, :], table[...])
    for dy in ORDER[:3]:
        halo_part(0, dy)
    source = wait_plane(0, ORDER[3])

    def keep(i, value):
        state[strip(i, BIG), :] = value

    finish_edges(
        pre,
        state,
        hot_halo.at[source],
        plane_rows(0, source),
        counts,
        w2[...],
        egain[0:1, :],
        eoff[0:1, :],
        hidden,
        edge_low,
        keep,
    )
    total = dot(hot_sum[...], edge_low[...])
    node[...] += node_finish(pv[...], total, v1[0, D:, :], v2[...], ngain[0:1, :], noff[0:1, :])
    exchange(1)
    tables(1)
    for i in range(NBIG):
        r = strip(i, BIG)
        pre[r, :] = 0.5 * (dot(edge_low[r, :], w1[1, :D, :]) + eb1[1:2, :]) + dot(hot_local[r, :], table[...])
    hot_last[...] = hot_halo[(y + 4 - ORDER[3]) % 4]
    wait_sends(0)
    for dy in ORDER[:3]:
        halo_part(1, dy)
    last_rows[...] = plane_rows(1, wait_plane(1, ORDER[3]))
    wait_sends(1)


def second_kernel(
    pre,
    state,
    node,
    pv,
    last_rows,
    hot_last,
    hot_sum,
    w2,
    v1,
    v2,
    counts,
    egain,
    eoff,
    ngain,
    noff,
    edge_out,
    node_out,
    result,
    hidden,
    low,
    out_sem,
):
    copies = []

    def put(i, value):
        result[strip(i, BIG), :] = value
        copies.append(
            pltpu.make_async_copy(
                result.at[pl.ds(i * BIG, BIG)], edge_out.at[pl.ds(i * BIG, BIG)], out_sem.at[i]
            )
        )
        copies[-1].start()

    finish_edges(
        pre,
        state,
        hot_last,
        last_rows[...],
        counts,
        w2[...],
        egain[1:2, :],
        eoff[1:2, :],
        hidden,
        low,
        put,
    )
    total = dot(hot_sum[...], low[...])
    node_out[...] = node[...] + node_finish(pv[...], total, v1[...], v2[...], ngain[1:2, :], noff[1:2, :])
    for c in copies:
        c.wait()


VMEM = pl.BlockSpec(memory_space=pltpu.VMEM)
SMEM = pl.BlockSpec(memory_space=pltpu.SMEM)
ANY = pl.BlockSpec(memory_space=pl.ANY)
HBM = pl.BlockSpec(memory_space=pltpu.HBM)


def shards(
    latents,
    edge_latents,
    edge_sender,
    edge_receiver,
    block_counts,
    send_rows,
    edge_first_weight,
    edge_first_bias,
    edge_second_weight,
    edge_gain,
    edge_offset,
    node_first_weight,
    node_first_bias,
    node_second_weight,
    node_gain,
    node_offset,
):
    snd = edge_sender.reshape(EDGE // 128, 128)
    rcv = edge_receiver.reshape(EDGE // 128, 128)
    lists = jnp.transpose(send_rows[0])
    shape = jax.ShapeDtypeStruct
    held = pl.pallas_call(
        first_kernel,
        out_shape=(
            pltpu.VMEM((EDGE, D), F32),
            pltpu.VMEM((EDGE, D), F32),
            pltpu.VMEM((ROWS, D), F32),
            pltpu.VMEM((ROWS, D), F32),
            pltpu.VMEM((256, D), BF16),
            pltpu.VMEM((EDGE, 256), BF16),
            pltpu.VMEM((ROWS, EDGE), BF16),
            pltpu.VMEM((D, D), BF16),
            pltpu.VMEM((D, D), BF16),
            pltpu.VMEM((D, D), BF16),
        ),
        in_specs=[HBM] * 16,
        out_specs=(VMEM,) * 10,
        scratch_shapes=[
            pltpu.VMEM((EDGE // 128, 128), jnp.int32),
            pltpu.VMEM((EDGE // 128, 128), jnp.int32),
            pltpu.SMEM((EDGE // 128,), jnp.int32),
            pltpu.VMEM((8, 128), jnp.int32),
        ]
        + [pltpu.VMEM((2, D), F32)] * 6
        + [
            pltpu.VMEM((2 * ROWS, HALF), F32),
            pltpu.VMEM((4, EDGE, 256), BF16),
            pltpu.VMEM((EDGE, 2 * ROWS), BF16),
            pltpu.VMEM((1024, ROWS), BF16),
            pltpu.VMEM((2, 3 * D, D), BF16),
            pltpu.VMEM((D, D), BF16),
            pltpu.VMEM((2, 2 * D, D), BF16),
            pltpu.VMEM((D, D), BF16),
            pltpu.VMEM((ROWS, HALF), BF16),
            pltpu.VMEM((ROWS, HALF), BF16),
            pltpu.VMEM((ROWS, D), BF16),
            pltpu.VMEM((EDGE, D), BF16),
            pltpu.VMEM((EDGE, D), BF16),
            pltpu.VMEM((2 * ROWS, D), BF16),
            pltpu.VMEM((2, 128, 8, D), BF16),
            pltpu.VMEM((2, 128, 8, D), BF16),
            pltpu.SemaphoreType.DMA,
            pltpu.SemaphoreType.DMA,
            pltpu.SemaphoreType.DMA((NBIG,)),
            pltpu.SemaphoreType.DMA((16,)),
            pltpu.SemaphoreType.DMA,
            pltpu.SemaphoreType.DMA,
            pltpu.SemaphoreType.DMA((2,)),
            pltpu.SemaphoreType.DMA((2, 4)),
            pltpu.SemaphoreType.REGULAR,
        ],
        compiler_params=pltpu.CompilerParams(
            collective_id=0, has_side_effects=True, vmem_limit_bytes=47 * 1024 * 1024
        ),
    )(
        latents,
        edge_latents,
        snd,
        rcv,
        block_counts,
        lists,
        edge_first_weight,
        edge_first_bias,
        edge_second_weight,
        edge_gain,
        edge_offset,
        node_first_weight,
        node_first_bias,
        node_second_weight,
        node_gain,
        node_offset,
    )
    new_edges, new_nodes = pl.pallas_call(
        second_kernel,
        out_shape=(shape((EDGE, D), F32), shape((ROWS, D), F32)),
        in_specs=[VMEM] * 10 + [SMEM] + [VMEM] * 4,
        out_specs=(ANY, VMEM),
        scratch_shapes=[
            pltpu.VMEM((EDGE, D), F32),
            pltpu.VMEM((EDGE, D), BF16),
            pltpu.VMEM((EDGE, D), BF16),
            pltpu.SemaphoreType.DMA((NBIG,)),
        ],
        compiler_params=pltpu.CompilerParams(vmem_limit_bytes=24 * 1024 * 1024),
    )(
        *held,
        block_counts,
        edge_gain,
        edge_offset,
        node_gain,
        node_offset,
    )
    return new_nodes, new_edges


def solution(mesh):
    split = P(("patch", "band"))
    return jax.shard_map(
        shards,
        mesh=mesh,
        in_specs=(
            P("patch", "band"),
            P(("patch", "band"), None),
            split,
            split,
            split,
            P(("patch", "band"), None, None),
        )
        + (P(),) * 10,
        out_specs=(P(("patch", "band"), None), P(("patch", "band"), None)),
        check_vma=False,
    )
```

```python
import functools

import jax
import jax.numpy as jnp
from jax import lax
from jax.experimental import pallas as pl
from jax.experimental.pallas import tpu as pltpu
from jax.sharding import PartitionSpec as P

MESH = pl.DeviceIdType.MESH
F32 = jnp.float32
BF16 = jnp.bfloat16
D = 512
HALF = 256
ROWS = 320
EDGE = 2560
BIG = 512
NBIG = EDGE // BIG
EPS = 1e-05
STEP = 37
UNSTEP = 45


def dot(a, b):
    return jnp.dot(a, b, preferred_element_type=F32)


def swish(v):
    half = 0.5 * v
    return half + half * jnp.tanh(half)


def norm(v, gain, offset):
    centre = v - jnp.sum(v, axis=-1, keepdims=True) * (1.0 / D)
    spread = jnp.sum(centre * centre, axis=-1, keepdims=True) * (1.0 / D)
    return centre * lax.rsqrt(spread + EPS) * gain + offset


def column(row):
    return jnp.transpose(jnp.broadcast_to(row, (128, 128)))


def hot(match):
    return jnp.where(match, 1.0, 0.0).astype(BF16)


def lanes(base):
    return (lax.broadcasted_iota(jnp.int32, (128, 128), 1) + base).astype(F32)


def strip(i, size):
    return slice(i * size, (i + 1) * size)


def finish_edges(pre, state, hot_last, rows, counts, w2, gain, offset, hidden, low, done):
    for i in range(NBIG):
        r = strip(i, BIG)
        half = pre[r, :] + dot(hot_last[r, :], rows)
        hidden[r, :] = (half + half * jnp.tanh(half)).astype(BF16)
    row = lax.broadcasted_iota(jnp.int32, (128, 1), 0)
    for i in range(NBIG):
        r = strip(i, BIG)
        n = BIG // 128
        usable = jnp.concatenate([row < counts[i * n + j] for j in range(n)], axis=0)
        update = norm(dot(hidden[r, :], w2), gain, offset)
        value = state[r, :] + jnp.where(usable, update, 0.0)
        low[r, :] = value.astype(BF16)
        done(i, value)


def node_finish(pv, summed, v1, w2, gain, offset):
    hidden = swish(pv + dot(summed.astype(BF16), v1)).astype(BF16)
    return norm(dot(hidden, w2), gain, offset)


def place():
    p = lax.axis_index("patch")
    b = lax.axis_index("band")
    core = p % 2
    z = (p // 2) % 4
    x = ((p // 8) % 2) * 2 + b
    y = p // 16
    return p, b, core, x, y, z


def at(core, x, y, z):
    return ((y * 2 + x // 2) * 4 + z) * 2 + core, x % 2


def apart(step):
    return step % 2, step // 2 % 4, step // 8 % 4, step // 32


def together(dc, dx, dy, dz):
    return dc % 2 + dx % 4 * 2 + dz % 4 * 8 + dy % 4 * 32


def number(core, x, y, z):
    patch, band = at(core % 2, x % 4, y % 4, z % 4)
    return patch * 2 + band


def first_kernel(
    latents,
    edges,
    snd_hbm,
    rcv_hbm,
    counts_hbm,
    lists_hbm,
    we1,
    eb1_hbm,
    we2,
    egain_hbm,
    eoff_hbm,
    wn1,
    nb1_hbm,
    wn2,
    ngain_hbm,
    noff_hbm,
    pre,
    state,
    node,
    pv,
    last_rows,
    hot_last,
    hot_sum,
    w2_next,
    v1_next,
    v2_next,
    snd,
    rcv,
    counts,
    lists,
    from_slot,
    eb1,
    egain,
    eoff,
    nb1,
    ngain,
    noff,
    lat,
    hot_halo,
    hot_local,
    hot_send,
    w1,
    w2,
    v1,
    v2,
    band_out,
    band_in,
    low,
    hidden,
    edge_low,
    table,
    stage,
    recv,
    list_sem,
    lat_sem,
    edge_sem,
    w_sem,
    band_send,
    band_recv,
    halo_send,
    halo_recv,
    greet,
):
    p, b, core, x, y, z = place()
    me = p * 2 + b
    barrier = pltpu.get_barrier_semaphore()
    plane = [(0, 0, dy, dz) for dy in range(4) for dz in range(4) if (dy, dz) != (0, 0)]
    line = [(dc, dx, 0, 0) for dc in range(2) for dx in range(4) if (dc, dx) != (0, 0)]

    def peer(dc, dx, dy, dz):
        return at((core + dc) % 2, (x + dx) % 4, (y + dy) % 4, (z + dz) % 4)

    lat_copy = pltpu.make_async_copy(latents, lat, lat_sem)
    lat_copy.start()
    list_copy = pltpu.make_async_copy(lists_hbm, lists, list_sem)
    list_copy.start()
    for o in line + plane:
        pl.semaphore_signal(barrier, inc=1, device_id=peer(*o), device_id_type=MESH)
    w_copies = [
        pltpu.make_async_copy(source, target, w_sem.at[i])
        for i, (source, target) in enumerate(
            (
                (we1, w1),
                (snd_hbm, snd),
                (rcv_hbm, rcv),
                (counts_hbm, counts),
                (eb1_hbm, eb1),
                (wn1, v1),
                (nb1_hbm, nb1),
                (we2.at[0], w2),
                (egain_hbm, egain),
                (eoff_hbm, eoff),
                (wn2.at[0], v2),
                (ngain_hbm, ngain),
                (noff_hbm, noff),
                (we2.at[1], w2_next),
                (wn1.at[1, pl.ds(D, D)], v1_next),
                (wn2.at[1], v2_next),
            )
        )
    ]
    edge_copies = [
        pltpu.make_async_copy(edges.at[pl.ds(i * BIG, BIG)], state.at[pl.ds(i * BIG, BIG)], edge_sem.at[i])
        for i in range(NBIG)
    ]

    lat_copy.wait()
    band_out[...] = lat[pl.ds((1 - b) * ROWS, ROWS), :].astype(BF16)
    for c in w_copies[:5] + edge_copies + w_copies[5:]:
        c.start()

    pl.semaphore_wait(barrier, len(plane) + len(line))
    for o in line:
        pl.semaphore_signal(greet, inc=1, device_id=peer(*o), device_id_type=MESH)
    band_copy = pltpu.make_async_remote_copy(
        src_ref=band_out,
        dst_ref=band_in,
        send_sem=band_send,
        recv_sem=band_recv,
        device_id=(p, 1 - b),
        device_id_type=MESH,
    )
    band_copy.start()

    list_copy.wait()
    step = lax.broadcasted_iota(jnp.int32, (1, 128), 1) * STEP % 128
    dc, dx, dz, dy = apart(step)
    asks = (lax.broadcasted_iota(jnp.int32, (128, 128), 0) == number(core + dc, x + dx, y + dy, z + dz)).astype(F32)
    asks = asks.astype(BF16)
    high = lists[...] // 256
    low_part = dot((lists[...] - 256 * high).astype(F32).astype(BF16), asks)
    wanted = 256.0 * dot(high.astype(F32).astype(BF16), asks) + low_part
    for c in range(8):
        block = jnp.concatenate(
            [jnp.broadcast_to(wanted[:, q : q + 1], (8, 128)) for q in range(16 * c, 16 * c + 16)], axis=0
        )
        for t in range(3):
            wide = 128 if t < 2 else 64
            hot_send[strip(c, 128), t * 128 : t * 128 + wide] = hot(block == lanes(t * 128))[:, :wide]

    w_copies[0].wait()
    band_copy.wait()
    own = lat[pl.ds(b * ROWS, ROWS), :]
    other = band_in[...].astype(F32)
    node[:, :HALF] = jnp.where(b == 0, own, other)
    node[:, HALF:] = jnp.where(b == 0, other, own)

    xs = [(x + d) % 4 for d in range(4)]

    def exchange(layer):
        low[...] = node[...].astype(BF16)
        table[:ROWS, :] = (0.5 * dot(low[...], w1[layer, D : 2 * D, :])).astype(BF16)

        def fill(c):
            chosen = dot(hot_send[strip(c, 256), :], table[:ROWS, :]).astype(BF16)
            stage[layer, strip(c, 32)] = chosen.reshape(32, 8, D)

        def send_part(c):
            def some(m, _):
                for i in range(16):
                    fixed = i * STEP % 128
                    dc, dx = fixed % 2, fixed // 2 % 4
                    turn = (m * (STEP * 16 % 128 // 16) + fixed // 16) % 8
                    dz, dy = turn % 2 * 2 + fixed // 8 % 2, turn // 2
                    px = (y + dy) % 4 * 16 + xs[dx] // 2 * 8 + (z + dz) % 4 * 2 + (core + dc) % 2

                    def send():
                        pltpu.make_async_remote_copy(
                            src_ref=stage.at[layer, m * 16 + i],
                            dst_ref=recv.at[layer, m * 16 + i],
                            send_sem=halo_send.at[layer],
                            recv_sem=halo_recv.at[layer, c],
                            device_id=(px, xs[dx] % 2),
                            device_id_type=MESH,
                        ).start()

                    if c == 0 and i == 0:
                        pl.when(m > 0)(send)
                    else:
                        send()
                return 0

            lax.fori_loop(2 * c, 2 * c + 2, some, 0)

        fill(0)
        if layer == 0:
            pl.semaphore_wait(greet, len(line))
        for c in range(4):
            if c < 3:
                fill(c + 1)
            send_part(c)
        recv[layer, 0] = stage[layer, 0]

    def tables(layer):
        table[ROWS:, :] = (0.5 * dot(low[...], w1[layer, 2 * D :, :])).astype(BF16)
        pv[...] = dot(low[...], v1[layer, :D, :]) + nb1[layer : layer + 1, :]

    def wait_part(layer, c):
        n = 31 if c == 0 else 32
        pltpu.make_async_copy(
            stage.at[layer, pl.ds(0, n)], recv.at[layer, pl.ds(0, n)], halo_recv.at[layer, c]
        ).wait()

    def part_rows(layer, c):
        return recv[layer, strip(c, 32)].reshape(256, D)

    def halo_part(layer, c):
        wait_part(layer, c)
        for i in range(NBIG):
            r = strip(i, BIG)
            pre[r, :] += dot(hot_halo[c, r, :], part_rows(layer, c))

    def wait_sends(layer):
        pltpu.make_async_copy(
            stage.at[layer, pl.ds(0, 127)], recv.at[layer, pl.ds(0, 127)], halo_send.at[layer]
        ).wait()

    exchange(0)
    for c in w_copies[1:5]:
        c.wait()

    remote = snd[...] - ROWS
    dev = remote // 8
    step = together(
        core - dev // 2 % 2 + 2,
        x - (dev // 16 % 2 * 2 + dev % 2) + 4,
        y - dev // 32 + 4,
        z - dev // 4 % 4 + 4,
    )
    place_of = ROWS + step * UNSTEP % 128 * 8 + remote % 8
    from_slot[...] = jnp.where(remote < 0, snd[...], place_of).astype(F32)

    def hots(i, _):
        rows = pl.ds(pl.multiple_of(i * 128, 128), 128)
        s = column(from_slot[pl.ds(i, 1), :])
        r = column(rcv[pl.ds(i, 1), :].astype(F32)) + float(ROWS)
        lane = lax.broadcasted_iota(jnp.int32, (128, 128), 1)
        mixed = jnp.where(lane < 64, s, r)
        for t, source in enumerate((s, s, mixed, r, r)):
            hot_local[rows, t * 128 : t * 128 + 128] = hot(source == lanes(t * 128))
        for t in range(8):
            part = hot(s == lanes(ROWS + t * 128))
            if t < 6:
                hot_halo[t // 2, rows, t % 2 * 128 : t % 2 * 128 + 128] = part
            else:
                hot_last[rows, t % 2 * 128 : t % 2 * 128 + 128] = part
        target = jnp.where(lane[:1] < counts[i], rcv[pl.ds(i, 1), :], -1)
        hot_sum[:, rows] = hot(lax.broadcasted_iota(jnp.int32, (ROWS, 128), 0) == target)
        return 0

    lax.fori_loop(0, EDGE // 128, hots, 0)
    for c in edge_copies + w_copies[5:]:
        c.wait()
    tables(0)
    for i in range(NBIG):
        r = strip(i, BIG)
        edge_part = 0.5 * (dot(state[r, :].astype(BF16), w1[0, :D, :]) + eb1[0:1, :])
        pre[r, :] = edge_part + dot(hot_local[r, :], table[...])
    for c in range(3):
        halo_part(0, c)
    wait_part(0, 3)

    def keep(i, value):
        state[strip(i, BIG), :] = value

    finish_edges(
        pre,
        state,
        hot_last,
        part_rows(0, 3),
        counts,
        w2[...],
        egain[0:1, :],
        eoff[0:1, :],
        hidden,
        edge_low,
        keep,
    )
    total = dot(hot_sum[...], edge_low[...])
    node[...] += node_finish(pv[...], total, v1[0, D:, :], v2[...], ngain[0:1, :], noff[0:1, :])
    exchange(1)
    tables(1)
    for i in range(NBIG):
        r = strip(i, BIG)
        pre[r, :] = 0.5 * (dot(edge_low[r, :], w1[1, :D, :]) + eb1[1:2, :]) + dot(hot_local[r, :], table[...])
    wait_sends(0)
    for c in range(3):
        halo_part(1, c)
    wait_part(1, 3)
    last_rows[...] = part_rows(1, 3)
    wait_sends(1)


def second_kernel(
    pre,
    state,
    node,
    pv,
    last_rows,
    hot_last,
    hot_sum,
    w2,
    v1,
    v2,
    counts,
    egain,
    eoff,
    ngain,
    noff,
    edge_out,
    node_out,
    result,
    hidden,
    low,
    out_sem,
):
    copies = []

    def put(i, value):
        result[strip(i, BIG), :] = value
        copies.append(
            pltpu.make_async_copy(
                result.at[pl.ds(i * BIG, BIG)], edge_out.at[pl.ds(i * BIG, BIG)], out_sem.at[i]
            )
        )
        copies[-1].start()

    finish_edges(
        pre,
        state,
        hot_last,
        last_rows[...],
        counts,
        w2[...],
        egain[1:2, :],
        eoff[1:2, :],
        hidden,
        low,
        put,
    )
    total = dot(hot_sum[...], low[...])
    node_out[...] = node[...] + node_finish(pv[...], total, v1[...], v2[...], ngain[1:2, :], noff[1:2, :])
    for c in copies:
        c.wait()


VMEM = pl.BlockSpec(memory_space=pltpu.VMEM)
SMEM = pl.BlockSpec(memory_space=pltpu.SMEM)
ANY = pl.BlockSpec(memory_space=pl.ANY)
HBM = pl.BlockSpec(memory_space=pltpu.HBM)


def shards(
    latents,
    edge_latents,
    edge_sender,
    edge_receiver,
    block_counts,
    send_rows,
    edge_first_weight,
    edge_first_bias,
    edge_second_weight,
    edge_gain,
    edge_offset,
    node_first_weight,
    node_first_bias,
    node_second_weight,
    node_gain,
    node_offset,
):
    snd = edge_sender.reshape(EDGE // 128, 128)
    rcv = edge_receiver.reshape(EDGE // 128, 128)
    lists = jnp.transpose(send_rows[0])
    shape = jax.ShapeDtypeStruct
    held = pl.pallas_call(
        first_kernel,
        out_shape=(
            pltpu.VMEM((EDGE, D), F32),
            pltpu.VMEM((EDGE, D), F32),
            pltpu.VMEM((ROWS, D), F32),
            pltpu.VMEM((ROWS, D), F32),
            pltpu.VMEM((256, D), BF16),
            pltpu.VMEM((EDGE, 256), BF16),
            pltpu.VMEM((ROWS, EDGE), BF16),
            pltpu.VMEM((D, D), BF16),
            pltpu.VMEM((D, D), BF16),
            pltpu.VMEM((D, D), BF16),
        ),
        in_specs=[HBM] * 16,
        out_specs=(VMEM,) * 10,
        scratch_shapes=[
            pltpu.VMEM((EDGE // 128, 128), jnp.int32),
            pltpu.VMEM((EDGE // 128, 128), jnp.int32),
            pltpu.SMEM((EDGE // 128,), jnp.int32),
            pltpu.VMEM((8, 128), jnp.int32),
            pltpu.VMEM((EDGE // 128, 128), F32),
        ]
        + [pltpu.VMEM((2, D), F32)] * 6
        + [
            pltpu.VMEM((2 * ROWS, HALF), F32),
            pltpu.VMEM((3, EDGE, 256), BF16),
            pltpu.VMEM((EDGE, 2 * ROWS), BF16),
            pltpu.VMEM((1024, ROWS), BF16),
            pltpu.VMEM((2, 3 * D, D), BF16),
            pltpu.VMEM((D, D), BF16),
            pltpu.VMEM((2, 2 * D, D), BF16),
            pltpu.VMEM((D, D), BF16),
            pltpu.VMEM((ROWS, HALF), BF16),
            pltpu.VMEM((ROWS, HALF), BF16),
            pltpu.VMEM((ROWS, D), BF16),
            pltpu.VMEM((EDGE, D), BF16),
            pltpu.VMEM((EDGE, D), BF16),
            pltpu.VMEM((2 * ROWS, D), BF16),
            pltpu.VMEM((2, 128, 8, D), BF16),
            pltpu.VMEM((2, 128, 8, D), BF16),
            pltpu.SemaphoreType.DMA,
            pltpu.SemaphoreType.DMA,
            pltpu.SemaphoreType.DMA((NBIG,)),
            pltpu.SemaphoreType.DMA((16,)),
            pltpu.SemaphoreType.DMA,
            pltpu.SemaphoreType.DMA,
            pltpu.SemaphoreType.DMA((2,)),
            pltpu.SemaphoreType.DMA((2, 4)),
            pltpu.SemaphoreType.REGULAR,
        ],
        compiler_params=pltpu.CompilerParams(
            collective_id=0, has_side_effects=True, vmem_limit_bytes=47 * 1024 * 1024
        ),
    )(
        latents,
        edge_latents,
        snd,
        rcv,
        block_counts,
        lists,
        edge_first_weight,
        edge_first_bias,
        edge_second_weight,
        edge_gain,
        edge_offset,
        node_first_weight,
        node_first_bias,
        node_second_weight,
        node_gain,
        node_offset,
    )
    new_edges, new_nodes = pl.pallas_call(
        second_kernel,
        out_shape=(shape((EDGE, D), F32), shape((ROWS, D), F32)),
        in_specs=[VMEM] * 10 + [SMEM] + [VMEM] * 4,
        out_specs=(ANY, VMEM),
        scratch_shapes=[
            pltpu.VMEM((EDGE, D), F32),
            pltpu.VMEM((EDGE, D), BF16),
            pltpu.VMEM((EDGE, D), BF16),
            pltpu.SemaphoreType.DMA((NBIG,)),
        ],
        compiler_params=pltpu.CompilerParams(vmem_limit_bytes=24 * 1024 * 1024),
    )(
        *held,
        block_counts,
        edge_gain,
        edge_offset,
        node_gain,
        node_offset,
    )
    return new_nodes, new_edges


def solution(mesh):
    split = P(("patch", "band"))
    return jax.shard_map(
        shards,
        mesh=mesh,
        in_specs=(
            P("patch", "band"),
            P(("patch", "band"), None),
            split,
            split,
            split,
            P(("patch", "band"), None, None),
        )
        + (P(),) * 10,
        out_specs=(P(("patch", "band"), None), P(("patch", "band"), None)),
        check_vma=False,
    )
```

```python
import functools

import jax
import jax.numpy as jnp
from jax import lax
from jax.experimental import pallas as pl
from jax.experimental.pallas import tpu as pltpu
from jax.sharding import PartitionSpec as P

MESH = pl.DeviceIdType.MESH
F32 = jnp.float32
BF16 = jnp.bfloat16
D = 512
HALF = 256
ROWS = 320
EDGE = 2560
BIG = 512
NBIG = EDGE // BIG
BLK = 256
PART = 64
EPS = 1e-05
STEP = 37
UNSTEP = 45


def dot(a, b):
    return jnp.dot(a, b, preferred_element_type=F32)


def swish(v):
    half = 0.5 * v
    return half + half * jnp.tanh(half)


def norm(v, gain, offset):
    centre = v - jnp.sum(v, axis=-1, keepdims=True) * (1.0 / D)
    spread = jnp.sum(centre * centre, axis=-1, keepdims=True) * (1.0 / D)
    return centre * lax.rsqrt(spread + EPS) * gain + offset


def column(row):
    return jnp.transpose(jnp.broadcast_to(row, (128, 128)))


def hot(match):
    return jnp.where(match, 1.0, 0.0).astype(BF16)


def lanes(base):
    return (lax.broadcasted_iota(jnp.int32, (128, 128), 1) + base).astype(F32)


def strip(i, size):
    return slice(i * size, (i + 1) * size)


def usable_rows(counts, block):
    row = lax.broadcasted_iota(jnp.int32, (128, 1), 0)
    n = BIG // 128
    return jnp.concatenate([row < counts[block * n + j] for j in range(n)], axis=0)


def finish_edges(pre, state, hot_last, rows, counts, w2, gain, hidden, product, low, out, done):
    for i in range(NBIG):
        r = strip(i, BIG)
        half = pre[r, :] + dot(hot_last[r, :], rows)
        hidden[r, :] = (half + half * jnp.tanh(half)).astype(BF16)
    row = lax.broadcasted_iota(jnp.int32, (PART, 1), 0)
    for i in range(EDGE // BLK):
        product[i % 2] = dot(hidden[strip(i, BLK), :], w2)
        for j in range(BLK // PART):
            first = i * BLK + j * PART
            r = slice(first, first + PART)
            value = product[i % 2, strip(j, PART), :]
            centre = value - jnp.sum(value, axis=-1, keepdims=True) * (1.0 / D)
            spread = jnp.sum(centre * centre, axis=-1, keepdims=True) * (1.0 / D)
            scale = jnp.where(row + first % 128 < counts[first // 128], lax.rsqrt(spread + EPS), 0.0)
            value = state[r, :] + centre * scale * gain
            out[r, :] = value
            low[r, :] = value.astype(BF16)
        done(i)


def finish_nodes(node, pv, total, v1, w2, gain, offset, done):
    summed = total.astype(BF16)
    parts = [strip(i, ROWS // 2) for i in range(2)]
    hidden = [swish(pv[r, :] + dot(summed[r, :], v1)).astype(BF16) for r in parts]
    results = [dot(h, w2) for h in hidden]
    for i in range(2):
        done(i, node[parts[i], :] + norm(results[i], gain, offset))


def place():
    p = lax.axis_index("patch")
    b = lax.axis_index("band")
    core = p % 2
    z = (p // 2) % 4
    x = ((p // 8) % 2) * 2 + b
    y = p // 16
    return p, b, core, x, y, z


def at(core, x, y, z):
    return ((y * 2 + x // 2) * 4 + z) * 2 + core, x % 2


def apart(step):
    return step % 2, step // 2 % 4, step // 8 % 4, step // 32


def together(dc, dx, dy, dz):
    return dc % 2 + dx % 4 * 2 + dz % 4 * 8 + dy % 4 * 32


def number(core, x, y, z):
    patch, band = at(core % 2, x % 4, y % 4, z % 4)
    return patch * 2 + band


def first_kernel(
    latents,
    edges,
    snd_hbm,
    rcv_hbm,
    counts_hbm,
    lists_hbm,
    we1,
    eb1_hbm,
    we2,
    egain_hbm,
    eoff_hbm,
    wn1,
    nb1_hbm,
    wn2,
    ngain_hbm,
    noff_hbm,
    pre,
    state,
    node,
    pv,
    last_rows,
    hot_last,
    hot_sum,
    w2_next,
    v1_next,
    v2_next,
    snd,
    rcv,
    counts,
    lists,
    from_slot,
    eb1,
    egain,
    eoff,
    nb1,
    ngain,
    noff,
    lat,
    hot_halo,
    hot_local,
    hot_send,
    w1,
    w2,
    v1,
    v2,
    band_out,
    band_in,
    low,
    hidden,
    product,
    edge_low,
    table,
    stage,
    recv,
    list_sem,
    lat_sem,
    edge_sem,
    w_sem,
    band_send,
    band_recv,
    halo_send,
    halo_recv,
    greet,
):
    p, b, core, x, y, z = place()
    me = p * 2 + b
    barrier = pltpu.get_barrier_semaphore()
    plane = [(0, 0, dy, dz) for dy in range(4) for dz in range(4) if (dy, dz) != (0, 0)]
    line = [(dc, dx, 0, 0) for dc in range(2) for dx in range(4) if (dc, dx) != (0, 0)]

    def peer(dc, dx, dy, dz):
        return at((core + dc) % 2, (x + dx) % 4, (y + dy) % 4, (z + dz) % 4)

    lat_copies = [
        pltpu.make_async_copy(latents.at[pl.ds(d * ROWS, ROWS)], lat.at[pl.ds(d * ROWS, ROWS)], lat_sem.at[i])
        for i, d in enumerate((1 - b, b))
    ]
    for c in lat_copies:
        c.start()
    list_copy = pltpu.make_async_copy(lists_hbm, lists, list_sem)
    list_copy.start()
    for o in line + plane:
        pl.semaphore_signal(barrier, inc=1, device_id=peer(*o), device_id_type=MESH)
    w_copies = [
        pltpu.make_async_copy(source, target, w_sem.at[i])
        for i, (source, target) in enumerate(
            (
                (we1, w1),
                (snd_hbm, snd),
                (rcv_hbm, rcv),
                (counts_hbm, counts),
                (eb1_hbm, eb1),
                (wn1, v1),
                (nb1_hbm, nb1),
                (we2.at[0], w2),
                (egain_hbm, egain),
                (eoff_hbm, eoff),
                (wn2.at[0], v2),
                (ngain_hbm, ngain),
                (noff_hbm, noff),
                (we2.at[1], w2_next),
                (wn1.at[1, pl.ds(D, D)], v1_next),
                (wn2.at[1], v2_next),
            )
        )
    ]
    edge_copies = [
        pltpu.make_async_copy(edges.at[pl.ds(i * BIG, BIG)], state.at[pl.ds(i * BIG, BIG)], edge_sem.at[i])
        for i in range(NBIG)
    ]

    lat_copies[0].wait()
    band_out[...] = lat[pl.ds((1 - b) * ROWS, ROWS), :].astype(BF16)
    for c in w_copies[:5] + edge_copies + w_copies[5:]:
        c.start()

    pl.semaphore_wait(barrier, len(plane) + len(line))
    for o in line:
        pl.semaphore_signal(greet, inc=1, device_id=peer(*o), device_id_type=MESH)
    band_copy = pltpu.make_async_remote_copy(
        src_ref=band_out,
        dst_ref=band_in,
        send_sem=band_send,
        recv_sem=band_recv,
        device_id=(p, 1 - b),
        device_id_type=MESH,
    )
    band_copy.start()

    list_copy.wait()
    step = lax.broadcasted_iota(jnp.int32, (1, 128), 1) * STEP % 128
    dc, dx, dz, dy = apart(step)
    asks = (lax.broadcasted_iota(jnp.int32, (128, 128), 0) == number(core + dc, x + dx, y + dy, z + dz)).astype(F32)
    asks = asks.astype(BF16)
    high = lists[...] // 256
    low_part = dot((lists[...] - 256 * high).astype(F32).astype(BF16), asks)
    wanted = 256.0 * dot(high.astype(F32).astype(BF16), asks) + low_part
    for c in range(8):
        block = jnp.concatenate(
            [jnp.broadcast_to(wanted[:, q : q + 1], (8, 128)) for q in range(16 * c, 16 * c + 16)], axis=0
        )
        for t in range(3):
            wide = 128 if t < 2 else 64
            hot_send[strip(c, 128), t * 128 : t * 128 + wide] = hot(block == lanes(t * 128))[:, :wide]

    w_copies[0].wait()
    lat_copies[1].wait()
    band_copy.wait()
    own = lat[pl.ds(b * ROWS, ROWS), :]
    other = band_in[...].astype(F32)
    node[:, :HALF] = jnp.where(b == 0, own, other)
    node[:, HALF:] = jnp.where(b == 0, other, own)

    xs = [(x + d) % 4 for d in range(4)]

    def exchange(layer):
        low[...] = node[...].astype(BF16)
        table[:ROWS, :] = (0.5 * dot(low[...], w1[layer, D : 2 * D, :])).astype(BF16)

        def fill(c):
            chosen = dot(hot_send[strip(c, 256), :], table[:ROWS, :]).astype(BF16)
            stage[layer, strip(c, 32)] = chosen.reshape(32, 8, D)

        def send_part(c):
            def some(m, _):
                for i in range(16):
                    fixed = i * STEP % 128
                    dc, dx = fixed % 2, fixed // 2 % 4
                    turn = (m * (STEP * 16 % 128 // 16) + fixed // 16) % 8
                    dz, dy = turn % 2 * 2 + fixed // 8 % 2, turn // 2
                    px = (y + dy) % 4 * 16 + xs[dx] // 2 * 8 + (z + dz) % 4 * 2 + (core + dc) % 2

                    def send():
                        pltpu.make_async_remote_copy(
                            src_ref=stage.at[layer, m * 16 + i],
                            dst_ref=recv.at[layer, m * 16 + i],
                            send_sem=halo_send.at[layer],
                            recv_sem=halo_recv.at[layer, c],
                            device_id=(px, xs[dx] % 2),
                            device_id_type=MESH,
                        ).start()

                    if c == 0 and i == 0:
                        pl.when(m > 0)(send)
                    else:
                        send()
                return 0

            lax.fori_loop(2 * c, 2 * c + 2, some, 0)

        fill(0)
        if layer == 0:
            pl.semaphore_wait(greet, len(line))
        for c in range(4):
            if c < 3:
                fill(c + 1)
            send_part(c)
        recv[layer, 0] = stage[layer, 0]

    def tables(layer):
        table[ROWS:, :] = (0.5 * dot(low[...], w1[layer, 2 * D :, :])).astype(BF16)
        pv[...] = dot(low[...], v1[layer, :D, :]) + nb1[layer : layer + 1, :]

    def wait_part(layer, c):
        n = 31 if c == 0 else 32
        pltpu.make_async_copy(
            stage.at[layer, pl.ds(0, n)], recv.at[layer, pl.ds(0, n)], halo_recv.at[layer, c]
        ).wait()

    def part_rows(layer, c):
        return recv[layer, strip(c, 32)].reshape(256, D)

    def halo_part(layer, c):
        wait_part(layer, c)
        for i in range(NBIG):
            r = strip(i, BIG)
            pre[r, :] += dot(hot_halo[c, r, :], part_rows(layer, c))

    def wait_sends(layer):
        pltpu.make_async_copy(
            stage.at[layer, pl.ds(0, 127)], recv.at[layer, pl.ds(0, 127)], halo_send.at[layer]
        ).wait()

    exchange(0)
    for c in w_copies[1:5]:
        c.wait()

    remote = snd[...] - ROWS
    dev = remote // 8
    step = together(
        core - dev // 2 % 2 + 2,
        x - (dev // 16 % 2 * 2 + dev % 2) + 4,
        y - dev // 32 + 4,
        z - dev // 4 % 4 + 4,
    )
    place_of = ROWS + step * UNSTEP % 128 * 8 + remote % 8
    from_slot[...] = jnp.where(remote < 0, snd[...], place_of).astype(F32)

    def hots(i, _):
        rows = pl.ds(pl.multiple_of(i * 128, 128), 128)
        s = column(from_slot[pl.ds(i, 1), :])
        r = column(rcv[pl.ds(i, 1), :].astype(F32)) + float(ROWS)
        lane = lax.broadcasted_iota(jnp.int32, (128, 128), 1)
        mixed = jnp.where(lane < 64, s, r)
        for t, source in enumerate((s, s, mixed, r, r)):
            hot_local[rows, t * 128 : t * 128 + 128] = hot(source == lanes(t * 128))
        for t in range(8):
            part = hot(s == lanes(ROWS + t * 128))
            if t < 6:
                hot_halo[t // 2, rows, t % 2 * 128 : t % 2 * 128 + 128] = part
            else:
                hot_last[rows, t % 2 * 128 : t % 2 * 128 + 128] = part
        target = jnp.where(lane[:1] < counts[i], rcv[pl.ds(i, 1), :], -1)
        hot_sum[:, rows] = hot(lax.broadcasted_iota(jnp.int32, (ROWS, 128), 0) == target)
        return 0

    lax.fori_loop(0, EDGE // 128, hots, 0)
    for c in edge_copies + w_copies[5:]:
        c.wait()
    tables(0)
    for i in range(NBIG):
        r = strip(i, BIG)
        edge_part = 0.5 * (dot(state[r, :].astype(BF16), w1[0, :D, :]) + eb1[0:1, :])
        pre[r, :] = edge_part + dot(hot_local[r, :], table[...])
        state[r, :] += jnp.where(usable_rows(counts, i), eoff[0:1, :], 0.0)
    for c in range(3):
        halo_part(0, c)
    wait_part(0, 3)

    finish_edges(
        pre,
        state,
        hot_last,
        part_rows(0, 3),
        counts,
        w2[...],
        egain[0:1, :],
        hidden,
        product,
        edge_low,
        state,
        lambda i: None,
    )

    def keep(i, value):
        node[strip(i, ROWS // 2), :] = value

    total = dot(hot_sum[...], edge_low[...])
    finish_nodes(node, pv, total, v1[0, D:, :], v2[...], ngain[0:1, :], noff[0:1, :], keep)
    exchange(1)
    tables(1)
    for i in range(NBIG):
        r = strip(i, BIG)
        pre[r, :] = 0.5 * (dot(edge_low[r, :], w1[1, :D, :]) + eb1[1:2, :]) + dot(hot_local[r, :], table[...])
        state[r, :] += jnp.where(usable_rows(counts, i), eoff[1:2, :], 0.0)
    wait_sends(0)
    for c in range(3):
        halo_part(1, c)
    wait_part(1, 3)
    last_rows[...] = part_rows(1, 3)
    wait_sends(1)


def second_kernel(
    pre,
    state,
    node,
    pv,
    last_rows,
    hot_last,
    hot_sum,
    w2,
    v1,
    v2,
    counts,
    egain,
    ngain,
    noff,
    edge_out,
    node_out,
    result,
    nodes,
    hidden,
    product,
    low,
    edge_sem,
    node_sem,
):
    copies = []

    def put(i):
        r = pl.ds(i * BLK, BLK)
        copies.append(pltpu.make_async_copy(result.at[r], edge_out.at[r], edge_sem.at[i]))
        copies[-1].start()

    def put_nodes(i, value):
        nodes[strip(i, ROWS // 2), :] = value
        r = pl.ds(i * (ROWS // 2), ROWS // 2)
        copies.append(pltpu.make_async_copy(nodes.at[r], node_out.at[r], node_sem.at[i]))
        copies[-1].start()

    finish_edges(
        pre,
        state,
        hot_last,
        last_rows[...],
        counts,
        w2[...],
        egain[1:2, :],
        hidden,
        product,
        low,
        result,
        put,
    )
    total = dot(hot_sum[...], low[...])
    finish_nodes(node, pv, total, v1[...], v2[...], ngain[1:2, :], noff[1:2, :], put_nodes)
    for c in copies:
        c.wait()


VMEM = pl.BlockSpec(memory_space=pltpu.VMEM)
SMEM = pl.BlockSpec(memory_space=pltpu.SMEM)
ANY = pl.BlockSpec(memory_space=pl.ANY)
HBM = pl.BlockSpec(memory_space=pltpu.HBM)


def shards(
    latents,
    edge_latents,
    edge_sender,
    edge_receiver,
    block_counts,
    send_rows,
    edge_first_weight,
    edge_first_bias,
    edge_second_weight,
    edge_gain,
    edge_offset,
    node_first_weight,
    node_first_bias,
    node_second_weight,
    node_gain,
    node_offset,
):
    snd = edge_sender.reshape(EDGE // 128, 128)
    rcv = edge_receiver.reshape(EDGE // 128, 128)
    lists = jnp.transpose(send_rows[0])
    shape = jax.ShapeDtypeStruct
    held = pl.pallas_call(
        first_kernel,
        out_shape=(
            pltpu.VMEM((EDGE, D), F32),
            pltpu.VMEM((EDGE, D), F32),
            pltpu.VMEM((ROWS, D), F32),
            pltpu.VMEM((ROWS, D), F32),
            pltpu.VMEM((256, D), BF16),
            pltpu.VMEM((EDGE, 256), BF16),
            pltpu.VMEM((ROWS, EDGE), BF16),
            pltpu.VMEM((D, D), BF16),
            pltpu.VMEM((D, D), BF16),
            pltpu.VMEM((D, D), BF16),
        ),
        in_specs=[HBM] * 16,
        out_specs=(VMEM,) * 10,
        scratch_shapes=[
            pltpu.VMEM((EDGE // 128, 128), jnp.int32),
            pltpu.VMEM((EDGE // 128, 128), jnp.int32),
            pltpu.SMEM((EDGE // 128,), jnp.int32),
            pltpu.VMEM((8, 128), jnp.int32),
            pltpu.VMEM((EDGE // 128, 128), F32),
        ]
        + [pltpu.VMEM((2, D), F32)] * 6
        + [
            pltpu.VMEM((2 * ROWS, HALF), F32),
            pltpu.VMEM((3, EDGE, 256), BF16),
            pltpu.VMEM((EDGE, 2 * ROWS), BF16),
            pltpu.VMEM((1024, ROWS), BF16),
            pltpu.VMEM((2, 3 * D, D), BF16),
            pltpu.VMEM((D, D), BF16),
            pltpu.VMEM((2, 2 * D, D), BF16),
            pltpu.VMEM((D, D), BF16),
            pltpu.VMEM((ROWS, HALF), BF16),
            pltpu.VMEM((ROWS, HALF), BF16),
            pltpu.VMEM((ROWS, D), BF16),
            pltpu.VMEM((EDGE, D), BF16),
            pltpu.VMEM((2, BLK, D), F32),
            pltpu.VMEM((EDGE, D), BF16),
            pltpu.VMEM((2 * ROWS, D), BF16),
            pltpu.VMEM((2, 128, 8, D), BF16),
            pltpu.VMEM((2, 128, 8, D), BF16),
            pltpu.SemaphoreType.DMA,
            pltpu.SemaphoreType.DMA((2,)),
            pltpu.SemaphoreType.DMA((NBIG,)),
            pltpu.SemaphoreType.DMA((16,)),
            pltpu.SemaphoreType.DMA,
            pltpu.SemaphoreType.DMA,
            pltpu.SemaphoreType.DMA((2,)),
            pltpu.SemaphoreType.DMA((2, 4)),
            pltpu.SemaphoreType.REGULAR,
        ],
        compiler_params=pltpu.CompilerParams(
            collective_id=0, has_side_effects=True, vmem_limit_bytes=47 * 1024 * 1024
        ),
    )(
        latents,
        edge_latents,
        snd,
        rcv,
        block_counts,
        lists,
        edge_first_weight,
        edge_first_bias,
        edge_second_weight,
        edge_gain,
        edge_offset,
        node_first_weight,
        node_first_bias,
        node_second_weight,
        node_gain,
        node_offset,
    )
    new_edges, new_nodes = pl.pallas_call(
        second_kernel,
        out_shape=(shape((EDGE, D), F32), shape((ROWS, D), F32)),
        in_specs=[VMEM] * 10 + [SMEM] + [VMEM] * 3,
        out_specs=(ANY, ANY),
        scratch_shapes=[
            pltpu.VMEM((EDGE, D), F32),
            pltpu.VMEM((ROWS, D), F32),
            pltpu.VMEM((EDGE, D), BF16),
            pltpu.VMEM((2, BLK, D), F32),
            pltpu.VMEM((EDGE, D), BF16),
            pltpu.SemaphoreType.DMA((EDGE // BLK,)),
            pltpu.SemaphoreType.DMA((2,)),
        ],
        compiler_params=pltpu.CompilerParams(vmem_limit_bytes=24 * 1024 * 1024),
    )(
        *held,
        block_counts,
        edge_gain,
        node_gain,
        node_offset,
    )
    return new_nodes, new_edges


def solution(mesh):
    split = P(("patch", "band"))
    return jax.shard_map(
        shards,
        mesh=mesh,
        in_specs=(
            P("patch", "band"),
            P(("patch", "band"), None),
            split,
            split,
            split,
            P(("patch", "band"), None, None),
        )
        + (P(),) * 10,
        out_specs=(P(("patch", "band"), None), P(("patch", "band"), None)),
        check_vma=False,
    )
```

```python
import functools

import jax
import jax.numpy as jnp
from jax import lax
from jax.experimental import pallas as pl
from jax.experimental.pallas import tpu as pltpu
from jax.sharding import PartitionSpec as P

MESH = pl.DeviceIdType.MESH
F32 = jnp.float32
BF16 = jnp.bfloat16
D = 512
HALF = 256
ROWS = 320
EDGE = 2560
BIG = 512
NBIG = EDGE // BIG
BLK = 256
PART = 64
EPS = 1e-05
STEP = 59
UNSTEP = 115


def dot(a, b):
    return jnp.dot(a, b, preferred_element_type=F32)


def swish(v):
    half = 0.5 * v
    return half + half * jnp.tanh(half)


def norm(v, gain, offset):
    centre = v - jnp.sum(v, axis=-1, keepdims=True) * (1.0 / D)
    spread = jnp.sum(centre * centre, axis=-1, keepdims=True) * (1.0 / D)
    return centre * lax.rsqrt(spread + EPS) * gain + offset


def column(row):
    return jnp.transpose(jnp.broadcast_to(row, (128, 128)))


def hot(match):
    return jnp.where(match, 1.0, 0.0).astype(BF16)


def lanes(base):
    return (lax.broadcasted_iota(jnp.int32, (128, 128), 1) + base).astype(F32)


def strip(i, size):
    return slice(i * size, (i + 1) * size)


def usable_rows(counts, block):
    row = lax.broadcasted_iota(jnp.int32, (128, 1), 0)
    n = BIG // 128
    return jnp.concatenate([row < counts[block * n + j] for j in range(n)], axis=0)


def finish_edges(pre, state, hot_last, rows, counts, w2, gain, hidden, product, low, out, done):
    for i in range(NBIG):
        r = strip(i, BIG)
        half = pre[r, :] + dot(hot_last[r, :], rows)
        hidden[r, :] = (half + half * jnp.tanh(half)).astype(BF16)
    row = lax.broadcasted_iota(jnp.int32, (PART, 1), 0)
    for i in range(EDGE // BLK):
        product[i % 2] = dot(hidden[strip(i, BLK), :], w2)
        for j in range(BLK // PART):
            first = i * BLK + j * PART
            r = slice(first, first + PART)
            value = product[i % 2, strip(j, PART), :]
            centre = value - jnp.sum(value, axis=-1, keepdims=True) * (1.0 / D)
            spread = jnp.sum(centre * centre, axis=-1, keepdims=True) * (1.0 / D)
            scale = jnp.where(row + first % 128 < counts[first // 128], lax.rsqrt(spread + EPS), 0.0)
            value = state[r, :] + centre * scale * gain
            out[r, :] = value
            low[r, :] = value.astype(BF16)
        done(i)


def finish_nodes(node, pv, hot_sum, edge_low, v1, w2, gain, offset, done):
    parts = [strip(i, ROWS // 2) for i in range(2)]
    sums = [dot(hot_sum[r, :], edge_low[...]).astype(BF16) for r in parts]
    hidden = [swish(pv[r, :] + dot(v, v1)).astype(BF16) for r, v in zip(parts, sums)]
    results = [dot(h, w2) for h in hidden]
    for i in range(2):
        done(i, node[parts[i], :] + norm(results[i], gain, offset))


def place():
    p = lax.axis_index("patch")
    b = lax.axis_index("band")
    core = p % 2
    z = (p // 2) % 4
    x = ((p // 8) % 2) * 2 + b
    y = p // 16
    return p, b, core, x, y, z


def at(core, x, y, z):
    return ((y * 2 + x // 2) * 4 + z) * 2 + core, x % 2


def apart(step):
    return step % 2, step // 2 % 4, step // 8 % 4, step // 32


def together(dc, dx, dy, dz):
    return dc % 2 + dx % 4 * 2 + dz % 4 * 8 + dy % 4 * 32


def number(core, x, y, z):
    patch, band = at(core % 2, x % 4, y % 4, z % 4)
    return patch * 2 + band


def first_kernel(
    latents,
    edges,
    snd_hbm,
    rcv_hbm,
    counts_hbm,
    lists_hbm,
    we1,
    eb1_hbm,
    we2,
    egain_hbm,
    eoff_hbm,
    wn1,
    nb1_hbm,
    wn2,
    ngain_hbm,
    noff_hbm,
    pre,
    state,
    node,
    pv,
    last_rows,
    hot_last,
    hot_sum,
    w2_next,
    v1_next,
    v2_next,
    snd,
    rcv,
    counts,
    lists,
    from_slot,
    eb1,
    egain,
    eoff,
    nb1,
    ngain,
    noff,
    lat,
    hot_halo,
    hot_local,
    hot_send,
    w1,
    w2,
    v1,
    v2,
    band_out,
    band_in,
    low,
    hidden,
    product,
    edge_low,
    table,
    stage,
    recv,
    list_sem,
    lat_sem,
    edge_sem,
    w_sem,
    band_send,
    band_recv,
    halo_send,
    halo_recv,
    greet,
):
    p, b, core, x, y, z = place()
    me = p * 2 + b
    barrier = pltpu.get_barrier_semaphore()
    plane = [(0, 0, dy, dz) for dy in range(4) for dz in range(4) if (dy, dz) != (0, 0)]
    line = [(dc, dx, 0, 0) for dc in range(2) for dx in range(4) if (dc, dx) != (0, 0)]

    def peer(dc, dx, dy, dz):
        return at((core + dc) % 2, (x + dx) % 4, (y + dy) % 4, (z + dz) % 4)

    half_rows = ROWS // 2
    lat_copies = []
    for i, d in enumerate((1 - b, 1 - b, b)):
        r = pl.ds(d * ROWS + (i % 2) * half_rows, half_rows) if i < 2 else pl.ds(d * ROWS, ROWS)
        lat_copies.append(pltpu.make_async_copy(latents.at[r], lat.at[r], lat_sem.at[i]))
        lat_copies[-1].start()
    list_copy = pltpu.make_async_copy(lists_hbm, lists, list_sem)
    list_copy.start()
    for o in line + plane:
        pl.semaphore_signal(barrier, inc=1, device_id=peer(*o), device_id_type=MESH)
    w_copies = [
        pltpu.make_async_copy(source, target, w_sem.at[i])
        for i, (source, target) in enumerate(
            (
                (we1, w1),
                (snd_hbm, snd),
                (rcv_hbm, rcv),
                (counts_hbm, counts),
                (eb1_hbm, eb1),
                (wn1, v1),
                (nb1_hbm, nb1),
                (we2.at[0], w2),
                (egain_hbm, egain),
                (eoff_hbm, eoff),
                (wn2.at[0], v2),
                (ngain_hbm, ngain),
                (noff_hbm, noff),
                (we2.at[1], w2_next),
                (wn1.at[1, pl.ds(D, D)], v1_next),
                (wn2.at[1], v2_next),
            )
        )
    ]
    edge_copies = [
        pltpu.make_async_copy(edges.at[pl.ds(i * BIG, BIG)], state.at[pl.ds(i * BIG, BIG)], edge_sem.at[i])
        for i in range(NBIG)
    ]

    for i in range(2):
        lat_copies[i].wait()
        band_out[strip(i, half_rows), :] = lat[pl.ds((1 - b) * ROWS + i * half_rows, half_rows), :].astype(BF16)
    for c in w_copies[:5] + edge_copies + w_copies[5:]:
        c.start()

    pl.semaphore_wait(barrier, len(plane) + len(line))
    for o in line:
        pl.semaphore_signal(greet, inc=1, device_id=peer(*o), device_id_type=MESH)
    band_copies = []
    for i in range(2):
        r = pl.ds(i * half_rows, half_rows)
        copy = pltpu.make_async_remote_copy(
            src_ref=band_out.at[r],
            dst_ref=band_in.at[r],
            send_sem=band_send.at[i],
            recv_sem=band_recv.at[i],
            device_id=(p, 1 - b),
            device_id_type=MESH,
        )
        copy.start()
        band_copies.append(copy)

    list_copy.wait()
    step = lax.broadcasted_iota(jnp.int32, (1, 128), 1) * STEP % 128
    dc, dx, dz, dy = apart(step)
    asks = (lax.broadcasted_iota(jnp.int32, (128, 128), 0) == number(core + dc, x + dx, y + dy, z + dz)).astype(F32)
    asks = asks.astype(BF16)
    high = lists[...] // 256
    low_part = dot((lists[...] - 256 * high).astype(F32).astype(BF16), asks)
    wanted = 256.0 * dot(high.astype(F32).astype(BF16), asks) + low_part
    for c in range(8):
        block = jnp.concatenate(
            [jnp.broadcast_to(wanted[:, q : q + 1], (8, 128)) for q in range(16 * c, 16 * c + 16)], axis=0
        )
        for t in range(3):
            wide = 128 if t < 2 else 64
            hot_send[strip(c, 128), t * 128 : t * 128 + wide] = hot(block == lanes(t * 128))[:, :wide]

    def project(layer, i):
        r = strip(i, half_rows)
        low[r, :] = node[r, :].astype(BF16)
        table[r, :] = (0.5 * dot(low[r, :], w1[layer, D : 2 * D, :])).astype(BF16)

    w_copies[0].wait()
    lat_copies[2].wait()
    for i in range(2):
        band_copies[i].wait()
        r = strip(i, half_rows)
        own = lat[pl.ds(b * ROWS + i * half_rows, half_rows), :]
        other = band_in[r, :].astype(F32)
        node[r, :HALF] = jnp.where(b == 0, own, other)
        node[r, HALF:] = jnp.where(b == 0, other, own)
        project(0, i)

    xs = [(x + d) % 4 for d in range(4)]

    def exchange(layer):
        def fill(first, last):
            chosen = dot(hot_send[first * 8 : last * 8, :], table[:ROWS, :]).astype(BF16)
            stage[layer, first:last] = chosen.reshape(last - first, 8, D)

        def send(first, last):
            for k in range(max(first, 1), last):
                dc, dx, dz, dy = apart(k * STEP % 128)
                px = (y + dy) % 4 * 16 + xs[dx] // 2 * 8 + (z + dz) % 4 * 2 + (core + dc) % 2
                pltpu.make_async_remote_copy(
                    src_ref=stage.at[layer, k],
                    dst_ref=recv.at[layer, k],
                    send_sem=halo_send.at[layer],
                    recv_sem=halo_recv.at[layer, k // 32],
                    device_id=(px, xs[dx] % 2),
                    device_id_type=MESH,
                ).start()

        cuts = (0, 16, 32, 64, 96, 128)
        fill(0, 16)
        if layer == 0:
            pl.semaphore_wait(greet, len(line))
        for i in range(1, 6):
            if i < 5:
                fill(cuts[i], cuts[i + 1])
            send(cuts[i - 1], cuts[i])
        recv[layer, 0] = stage[layer, 0]

    def tables(layer):
        table[ROWS:, :] = (0.5 * dot(low[...], w1[layer, 2 * D :, :])).astype(BF16)
        pv[...] = dot(low[...], v1[layer, :D, :]) + nb1[layer : layer + 1, :]

    def wait_part(layer, c):
        n = 31 if c == 0 else 32
        pltpu.make_async_copy(
            stage.at[layer, pl.ds(0, n)], recv.at[layer, pl.ds(0, n)], halo_recv.at[layer, c]
        ).wait()

    def part_rows(layer, c):
        return recv[layer, strip(c, 32)].reshape(256, D)

    def halo_part(layer, c):
        wait_part(layer, c)
        for i in range(NBIG):
            r = strip(i, BIG)
            pre[r, :] += dot(hot_halo[c, r, :], part_rows(layer, c))

    def wait_sends(layer):
        pltpu.make_async_copy(
            stage.at[layer, pl.ds(0, 127)], recv.at[layer, pl.ds(0, 127)], halo_send.at[layer]
        ).wait()

    exchange(0)
    for c in w_copies[1:5]:
        c.wait()

    remote = snd[...] - ROWS
    dev = remote // 8
    step = together(
        core - dev // 2 % 2 + 2,
        x - (dev // 16 % 2 * 2 + dev % 2) + 4,
        y - dev // 32 + 4,
        z - dev // 4 % 4 + 4,
    )
    place_of = ROWS + step * UNSTEP % 128 * 8 + remote % 8
    from_slot[...] = jnp.where(remote < 0, snd[...], place_of).astype(F32)

    def hots(i, _):
        rows = pl.ds(pl.multiple_of(i * 128, 128), 128)
        s = column(from_slot[pl.ds(i, 1), :])
        r = column(rcv[pl.ds(i, 1), :].astype(F32)) + float(ROWS)
        lane = lax.broadcasted_iota(jnp.int32, (128, 128), 1)
        mixed = jnp.where(lane < 64, s, r)
        for t, source in enumerate((s, s, mixed, r, r)):
            hot_local[rows, t * 128 : t * 128 + 128] = hot(source == lanes(t * 128))
        for t in range(8):
            part = hot(s == lanes(ROWS + t * 128))
            if t < 6:
                hot_halo[t // 2, rows, t % 2 * 128 : t % 2 * 128 + 128] = part
            else:
                hot_last[rows, t % 2 * 128 : t % 2 * 128 + 128] = part
        target = jnp.where(lane[:1] < counts[i], rcv[pl.ds(i, 1), :], -1)
        hot_sum[:, rows] = hot(lax.broadcasted_iota(jnp.int32, (ROWS, 128), 0) == target)
        return 0

    lax.fori_loop(0, EDGE // 128, hots, 0)
    for c in edge_copies + w_copies[5:]:
        c.wait()
    tables(0)
    for i in range(NBIG):
        r = strip(i, BIG)
        edge_part = 0.5 * (dot(state[r, :].astype(BF16), w1[0, :D, :]) + eb1[0:1, :])
        pre[r, :] = edge_part + dot(hot_local[r, :], table[...])
        state[r, :] += jnp.where(usable_rows(counts, i), eoff[0:1, :], 0.0)
    for c in range(3):
        halo_part(0, c)
    wait_part(0, 3)

    finish_edges(
        pre,
        state,
        hot_last,
        part_rows(0, 3),
        counts,
        w2[...],
        egain[0:1, :],
        hidden,
        product,
        edge_low,
        state,
        lambda i: None,
    )

    def keep(i, value):
        node[strip(i, ROWS // 2), :] = value
        project(1, i)

    finish_nodes(node, pv, hot_sum, edge_low, v1[0, D:, :], v2[...], ngain[0:1, :], noff[0:1, :], keep)
    exchange(1)
    tables(1)
    for i in range(NBIG):
        r = strip(i, BIG)
        pre[r, :] = 0.5 * (dot(edge_low[r, :], w1[1, :D, :]) + eb1[1:2, :]) + dot(hot_local[r, :], table[...])
        state[r, :] += jnp.where(usable_rows(counts, i), eoff[1:2, :], 0.0)
    wait_sends(0)
    for c in range(3):
        halo_part(1, c)
    wait_part(1, 3)
    last_rows[...] = part_rows(1, 3)
    wait_sends(1)


def second_kernel(
    pre,
    state,
    node,
    pv,
    last_rows,
    hot_last,
    hot_sum,
    w2,
    v1,
    v2,
    counts,
    egain,
    ngain,
    noff,
    edge_out,
    node_out,
    result,
    nodes,
    hidden,
    product,
    low,
    edge_sem,
    node_sem,
):
    copies = []

    def put(i):
        r = pl.ds(i * BLK, BLK)
        copies.append(pltpu.make_async_copy(result.at[r], edge_out.at[r], edge_sem.at[i]))
        copies[-1].start()

    def put_nodes(i, value):
        nodes[strip(i, ROWS // 2), :] = value
        r = pl.ds(i * (ROWS // 2), ROWS // 2)
        copies.append(pltpu.make_async_copy(nodes.at[r], node_out.at[r], node_sem.at[i]))
        copies[-1].start()

    finish_edges(
        pre,
        state,
        hot_last,
        last_rows[...],
        counts,
        w2[...],
        egain[1:2, :],
        hidden,
        product,
        low,
        result,
        put,
    )
    finish_nodes(node, pv, hot_sum, low, v1[...], v2[...], ngain[1:2, :], noff[1:2, :], put_nodes)
    for c in copies:
        c.wait()


VMEM = pl.BlockSpec(memory_space=pltpu.VMEM)
SMEM = pl.BlockSpec(memory_space=pltpu.SMEM)
ANY = pl.BlockSpec(memory_space=pl.ANY)
HBM = pl.BlockSpec(memory_space=pltpu.HBM)


def shards(
    latents,
    edge_latents,
    edge_sender,
    edge_receiver,
    block_counts,
    send_rows,
    edge_first_weight,
    edge_first_bias,
    edge_second_weight,
    edge_gain,
    edge_offset,
    node_first_weight,
    node_first_bias,
    node_second_weight,
    node_gain,
    node_offset,
):
    snd = edge_sender.reshape(EDGE // 128, 128)
    rcv = edge_receiver.reshape(EDGE // 128, 128)
    lists = jnp.transpose(send_rows[0])
    shape = jax.ShapeDtypeStruct
    held = pl.pallas_call(
        first_kernel,
        out_shape=(
            pltpu.VMEM((EDGE, D), F32),
            pltpu.VMEM((EDGE, D), F32),
            pltpu.VMEM((ROWS, D), F32),
            pltpu.VMEM((ROWS, D), F32),
            pltpu.VMEM((256, D), BF16),
            pltpu.VMEM((EDGE, 256), BF16),
            pltpu.VMEM((ROWS, EDGE), BF16),
            pltpu.VMEM((D, D), BF16),
            pltpu.VMEM((D, D), BF16),
            pltpu.VMEM((D, D), BF16),
        ),
        in_specs=[HBM] * 16,
        out_specs=(VMEM,) * 10,
        scratch_shapes=[
            pltpu.VMEM((EDGE // 128, 128), jnp.int32),
            pltpu.VMEM((EDGE // 128, 128), jnp.int32),
            pltpu.SMEM((EDGE // 128,), jnp.int32),
            pltpu.VMEM((8, 128), jnp.int32),
            pltpu.VMEM((EDGE // 128, 128), F32),
        ]
        + [pltpu.VMEM((2, D), F32)] * 6
        + [
            pltpu.VMEM((2 * ROWS, HALF), F32),
            pltpu.VMEM((3, EDGE, 256), BF16),
            pltpu.VMEM((EDGE, 2 * ROWS), BF16),
            pltpu.VMEM((1024, ROWS), BF16),
            pltpu.VMEM((2, 3 * D, D), BF16),
            pltpu.VMEM((D, D), BF16),
            pltpu.VMEM((2, 2 * D, D), BF16),
            pltpu.VMEM((D, D), BF16),
            pltpu.VMEM((ROWS, HALF), BF16),
            pltpu.VMEM((ROWS, HALF), BF16),
            pltpu.VMEM((ROWS, D), BF16),
            pltpu.VMEM((EDGE, D), BF16),
            pltpu.VMEM((2, BLK, D), F32),
            pltpu.VMEM((EDGE, D), BF16),
            pltpu.VMEM((2 * ROWS, D), BF16),
            pltpu.VMEM((2, 128, 8, D), BF16),
            pltpu.VMEM((2, 128, 8, D), BF16),
            pltpu.SemaphoreType.DMA,
            pltpu.SemaphoreType.DMA((3,)),
            pltpu.SemaphoreType.DMA((NBIG,)),
            pltpu.SemaphoreType.DMA((16,)),
            pltpu.SemaphoreType.DMA((2,)),
            pltpu.SemaphoreType.DMA((2,)),
            pltpu.SemaphoreType.DMA((2,)),
            pltpu.SemaphoreType.DMA((2, 4)),
            pltpu.SemaphoreType.REGULAR,
        ],
        compiler_params=pltpu.CompilerParams(
            collective_id=0, has_side_effects=True, vmem_limit_bytes=47 * 1024 * 1024
        ),
    )(
        latents,
        edge_latents,
        snd,
        rcv,
        block_counts,
        lists,
        edge_first_weight,
        edge_first_bias,
        edge_second_weight,
        edge_gain,
        edge_offset,
        node_first_weight,
        node_first_bias,
        node_second_weight,
        node_gain,
        node_offset,
    )
    new_edges, new_nodes = pl.pallas_call(
        second_kernel,
        out_shape=(shape((EDGE, D), F32), shape((ROWS, D), F32)),
        in_specs=[VMEM] * 10 + [SMEM] + [VMEM] * 3,
        out_specs=(ANY, ANY),
        scratch_shapes=[
            pltpu.VMEM((EDGE, D), F32),
            pltpu.VMEM((ROWS, D), F32),
            pltpu.VMEM((EDGE, D), BF16),
            pltpu.VMEM((2, BLK, D), F32),
            pltpu.VMEM((EDGE, D), BF16),
            pltpu.SemaphoreType.DMA((EDGE // BLK,)),
            pltpu.SemaphoreType.DMA((2,)),
        ],
        compiler_params=pltpu.CompilerParams(vmem_limit_bytes=24 * 1024 * 1024),
    )(
        *held,
        block_counts,
        edge_gain,
        node_gain,
        node_offset,
    )
    return new_nodes, new_edges


def solution(mesh):
    split = P(("patch", "band"))
    return jax.shard_map(
        shards,
        mesh=mesh,
        in_specs=(
            P("patch", "band"),
            P(("patch", "band"), None),
            split,
            split,
            split,
            P(("patch", "band"), None, None),
        )
        + (P(),) * 10,
        out_specs=(P(("patch", "band"), None), P(("patch", "band"), None)),
        check_vma=False,
    )
```

```python
import functools

import jax
import jax.numpy as jnp
from jax import lax
from jax.experimental import pallas as pl
from jax.experimental.pallas import tpu as pltpu
from jax.sharding import PartitionSpec as P

MESH = pl.DeviceIdType.MESH
F32 = jnp.float32
BF16 = jnp.bfloat16
D = 512
HALF = 256
ROWS = 320
EDGE = 2560
BIG = 512
NBIG = EDGE // BIG
BLK = 256
PART = 64
EPS = 1e-05
STEP = 59
UNSTEP = 115


def dot(a, b):
    return jnp.dot(a, b, preferred_element_type=F32)


def swish(v):
    half = 0.5 * v
    return half + half * jnp.tanh(half)


def norm(v, gain, offset):
    centre = v - jnp.sum(v, axis=-1, keepdims=True) * (1.0 / D)
    spread = jnp.sum(centre * centre, axis=-1, keepdims=True) * (1.0 / D)
    return centre * lax.rsqrt(spread + EPS) * gain + offset


def column(row):
    return jnp.transpose(jnp.broadcast_to(row, (128, 128)))


def hot(match):
    return jnp.where(match, 1.0, 0.0).astype(BF16)


def lanes(base):
    return (lax.broadcasted_iota(jnp.int32, (128, 128), 1) + base).astype(F32)


def strip(i, size):
    return slice(i * size, (i + 1) * size)


def usable_rows(counts, block):
    row = lax.broadcasted_iota(jnp.int32, (128, 1), 0)
    n = BIG // 128
    return jnp.concatenate([row < counts[block * n + j] for j in range(n)], axis=0)


def finish_edges(pre, state, hot_last, rows, counts, w2, gain, hidden, product, low, out, done):
    for i in range(NBIG):
        r = strip(i, BIG)
        half = pre[r, :] + dot(hot_last[r, :], rows)
        hidden[r, :] = (half + half * jnp.tanh(half)).astype(BF16)
    row = lax.broadcasted_iota(jnp.int32, (PART, 1), 0)
    for i in range(EDGE // BLK):
        product[i % 2] = dot(hidden[strip(i, BLK), :], w2)
        for j in range(BLK // PART):
            first = i * BLK + j * PART
            r = slice(first, first + PART)
            value = product[i % 2, strip(j, PART), :]
            centre = value - jnp.sum(value, axis=-1, keepdims=True) * (1.0 / D)
            spread = jnp.sum(centre * centre, axis=-1, keepdims=True) * (1.0 / D)
            scale = jnp.where(row + first % 128 < counts[first // 128], lax.rsqrt(spread + EPS), 0.0)
            value = state[r, :] + centre * scale * gain
            out[r, :] = value
            low[r, :] = value.astype(BF16)
        done(i)


def finish_nodes(node, pv, hot_sum, edge_low, v1, w2, gain, offset, done):
    parts = [strip(i, ROWS // 2) for i in range(2)]
    sums = [dot(hot_sum[r, :], edge_low[...]).astype(BF16) for r in parts]
    hidden = [swish(pv[r, :] + dot(v, v1)).astype(BF16) for r, v in zip(parts, sums)]
    results = [dot(h, w2) for h in hidden]
    for i in range(2):
        done(i, node[parts[i], :] + norm(results[i], gain, offset))


def place():
    p = lax.axis_index("patch")
    b = lax.axis_index("band")
    core = p % 2
    z = (p // 2) % 4
    x = ((p // 8) % 2) * 2 + b
    y = p // 16
    return p, b, core, x, y, z


def at(core, x, y, z):
    return ((y * 2 + x // 2) * 4 + z) * 2 + core, x % 2


def apart(step):
    return step % 2, step // 2 % 4, step // 8 % 4, step // 32


def together(dc, dx, dy, dz):
    return dc % 2 + dx % 4 * 2 + dz % 4 * 8 + dy % 4 * 32


def distance(k):
    return sum(min(d, 4 - d) for d in apart(k * STEP % 128)[1:])


def number(core, x, y, z):
    patch, band = at(core % 2, x % 4, y % 4, z % 4)
    return patch * 2 + band


def first_kernel(
    latents,
    edges,
    snd_hbm,
    rcv_hbm,
    counts_hbm,
    lists_hbm,
    we1,
    eb1_hbm,
    we2,
    egain_hbm,
    eoff_hbm,
    wn1,
    nb1_hbm,
    wn2,
    ngain_hbm,
    noff_hbm,
    pre,
    state,
    node,
    pv,
    last_rows,
    hot_last,
    hot_sum,
    w2_next,
    v1_next,
    v2_next,
    snd,
    rcv,
    counts,
    lists,
    from_slot,
    eb1,
    egain,
    eoff,
    nb1,
    ngain,
    noff,
    lat,
    hot_halo,
    hot_local,
    hot_send,
    w1,
    w2,
    v1,
    v2,
    band_out,
    band_in,
    low,
    hidden,
    product,
    edge_low,
    table,
    stage,
    recv,
    list_sem,
    lat_sem,
    edge_sem,
    w_sem,
    band_send,
    band_recv,
    halo_send,
    halo_recv,
    greet,
):
    p, b, core, x, y, z = place()
    me = p * 2 + b
    barrier = pltpu.get_barrier_semaphore()
    plane = [(0, 0, dy, dz) for dy in range(4) for dz in range(4) if (dy, dz) != (0, 0)]
    line = [(dc, dx, 0, 0) for dc in range(2) for dx in range(4) if (dc, dx) != (0, 0)]

    def peer(dc, dx, dy, dz):
        return at((core + dc) % 2, (x + dx) % 4, (y + dy) % 4, (z + dz) % 4)

    half_rows = ROWS // 2
    lat_copies = []
    for i, d in enumerate((1 - b, 1 - b, b)):
        r = pl.ds(d * ROWS + (i % 2) * half_rows, half_rows) if i < 2 else pl.ds(d * ROWS, ROWS)
        lat_copies.append(pltpu.make_async_copy(latents.at[r], lat.at[r], lat_sem.at[i]))
        lat_copies[-1].start()
    list_copy = pltpu.make_async_copy(lists_hbm, lists, list_sem)
    list_copy.start()
    for o in line + plane:
        pl.semaphore_signal(barrier, inc=1, device_id=peer(*o), device_id_type=MESH)
    w_copies = [
        pltpu.make_async_copy(source, target, w_sem.at[i])
        for i, (source, target) in enumerate(
            (
                (we1, w1),
                (snd_hbm, snd),
                (rcv_hbm, rcv),
                (counts_hbm, counts),
                (eb1_hbm, eb1),
                (wn1, v1),
                (nb1_hbm, nb1),
                (we2.at[0], w2),
                (egain_hbm, egain),
                (eoff_hbm, eoff),
                (wn2.at[0], v2),
                (ngain_hbm, ngain),
                (noff_hbm, noff),
                (we2.at[1], w2_next),
                (wn1.at[1, pl.ds(D, D)], v1_next),
                (wn2.at[1], v2_next),
            )
        )
    ]
    edge_copies = [
        pltpu.make_async_copy(edges.at[pl.ds(i * BIG, BIG)], state.at[pl.ds(i * BIG, BIG)], edge_sem.at[i])
        for i in range(NBIG)
    ]

    for i in range(2):
        lat_copies[i].wait()
        band_out[strip(i, half_rows), :] = lat[pl.ds((1 - b) * ROWS + i * half_rows, half_rows), :].astype(BF16)
    for c in w_copies[:5] + edge_copies + w_copies[5:]:
        c.start()

    pl.semaphore_wait(barrier, len(plane) + len(line))
    for o in line:
        pl.semaphore_signal(greet, inc=1, device_id=peer(*o), device_id_type=MESH)
    band_copies = []
    for i in range(2):
        r = pl.ds(i * half_rows, half_rows)
        copy = pltpu.make_async_remote_copy(
            src_ref=band_out.at[r],
            dst_ref=band_in.at[r],
            send_sem=band_send.at[i],
            recv_sem=band_recv.at[i],
            device_id=(p, 1 - b),
            device_id_type=MESH,
        )
        copy.start()
        band_copies.append(copy)

    list_copy.wait()
    step = lax.broadcasted_iota(jnp.int32, (1, 128), 1) * STEP % 128
    dc, dx, dz, dy = apart(step)
    asks = (lax.broadcasted_iota(jnp.int32, (128, 128), 0) == number(core + dc, x + dx, y + dy, z + dz)).astype(F32)
    asks = asks.astype(BF16)
    high = lists[...] // 256
    low_part = dot((lists[...] - 256 * high).astype(F32).astype(BF16), asks)
    wanted = 256.0 * dot(high.astype(F32).astype(BF16), asks) + low_part
    for c in range(8):
        block = jnp.concatenate(
            [jnp.broadcast_to(wanted[:, q : q + 1], (8, 128)) for q in range(16 * c, 16 * c + 16)], axis=0
        )
        for t in range(3):
            wide = 128 if t < 2 else 64
            hot_send[strip(c, 128), t * 128 : t * 128 + wide] = hot(block == lanes(t * 128))[:, :wide]

    def project(layer, i):
        r = strip(i, half_rows)
        low[r, :] = node[r, :].astype(BF16)
        table[r, :] = (0.5 * dot(low[r, :], w1[layer, D : 2 * D, :])).astype(BF16)

    w_copies[0].wait()
    lat_copies[2].wait()
    for i in range(2):
        band_copies[i].wait()
        r = strip(i, half_rows)
        own = lat[pl.ds(b * ROWS + i * half_rows, half_rows), :]
        other = band_in[r, :].astype(F32)
        node[r, :HALF] = jnp.where(b == 0, own, other)
        node[r, HALF:] = jnp.where(b == 0, other, own)
        project(0, i)

    xs = [(x + d) % 4 for d in range(4)]

    def exchange(layer):
        def fill(first, last):
            chosen = dot(hot_send[first * 8 : last * 8, :], table[:ROWS, :]).astype(BF16)
            stage[layer, first:last] = chosen.reshape(last - first, 8, D)

        def send(first, last):
            for k in sorted(range(max(first, 1), last), key=lambda k: -distance(k)):
                dc, dx, dz, dy = apart(k * STEP % 128)
                px = (y + dy) % 4 * 16 + xs[dx] // 2 * 8 + (z + dz) % 4 * 2 + (core + dc) % 2
                pltpu.make_async_remote_copy(
                    src_ref=stage.at[layer, k],
                    dst_ref=recv.at[layer, k],
                    send_sem=halo_send.at[layer],
                    recv_sem=halo_recv.at[layer, k // 32],
                    device_id=(px, xs[dx] % 2),
                    device_id_type=MESH,
                ).start()

        cuts = (0, 16, 32, 64, 96, 128)
        fill(0, 16)
        if layer == 0:
            pl.semaphore_wait(greet, len(line))
        for i in range(1, 6):
            if i < 5:
                fill(cuts[i], cuts[i + 1])
            send(cuts[i - 1], cuts[i])
        recv[layer, 0] = stage[layer, 0]

    def tables(layer):
        table[ROWS:, :] = (0.5 * dot(low[...], w1[layer, 2 * D :, :])).astype(BF16)
        pv[...] = dot(low[...], v1[layer, :D, :]) + nb1[layer : layer + 1, :]

    def wait_part(layer, c):
        n = 31 if c == 0 else 32
        pltpu.make_async_copy(
            stage.at[layer, pl.ds(0, n)], recv.at[layer, pl.ds(0, n)], halo_recv.at[layer, c]
        ).wait()

    def part_rows(layer, c):
        return recv[layer, strip(c, 32)].reshape(256, D)

    def halo_part(layer, c):
        wait_part(layer, c)
        for i in range(NBIG):
            r = strip(i, BIG)
            pre[r, :] += dot(hot_halo[c, r, :], part_rows(layer, c))

    def wait_sends(layer):
        pltpu.make_async_copy(
            stage.at[layer, pl.ds(0, 127)], recv.at[layer, pl.ds(0, 127)], halo_send.at[layer]
        ).wait()

    exchange(0)
    for c in w_copies[1:5]:
        c.wait()

    remote = snd[...] - ROWS
    dev = remote // 8
    step = together(
        core - dev // 2 % 2 + 2,
        x - (dev // 16 % 2 * 2 + dev % 2) + 4,
        y - dev // 32 + 4,
        z - dev // 4 % 4 + 4,
    )
    place_of = ROWS + step * UNSTEP % 128 * 8 + remote % 8
    from_slot[...] = jnp.where(remote < 0, snd[...], place_of).astype(F32)

    def hots(i, _):
        rows = pl.ds(pl.multiple_of(i * 128, 128), 128)
        s = column(from_slot[pl.ds(i, 1), :])
        r = column(rcv[pl.ds(i, 1), :].astype(F32)) + float(ROWS)
        lane = lax.broadcasted_iota(jnp.int32, (128, 128), 1)
        mixed = jnp.where(lane < 64, s, r)
        for t, source in enumerate((s, s, mixed, r, r)):
            hot_local[rows, t * 128 : t * 128 + 128] = hot(source == lanes(t * 128))
        for t in range(8):
            part = hot(s == lanes(ROWS + t * 128))
            if t < 6:
                hot_halo[t // 2, rows, t % 2 * 128 : t % 2 * 128 + 128] = part
            else:
                hot_last[rows, t % 2 * 128 : t % 2 * 128 + 128] = part
        target = jnp.where(lane[:1] < counts[i], rcv[pl.ds(i, 1), :], -1)
        hot_sum[:, rows] = hot(lax.broadcasted_iota(jnp.int32, (ROWS, 128), 0) == target)
        return 0

    lax.fori_loop(0, EDGE // 128, hots, 0)
    for c in edge_copies + w_copies[5:]:
        c.wait()
    tables(0)
    for i in range(NBIG):
        r = strip(i, BIG)
        edge_part = 0.5 * (dot(state[r, :].astype(BF16), w1[0, :D, :]) + eb1[0:1, :])
        pre[r, :] = edge_part + dot(hot_local[r, :], table[...])
        state[r, :] += jnp.where(usable_rows(counts, i), eoff[0:1, :], 0.0)
    for c in range(3):
        halo_part(0, c)
    wait_part(0, 3)

    finish_edges(
        pre,
        state,
        hot_last,
        part_rows(0, 3),
        counts,
        w2[...],
        egain[0:1, :],
        hidden,
        product,
        edge_low,
        state,
        lambda i: None,
    )

    def keep(i, value):
        node[strip(i, ROWS // 2), :] = value
        project(1, i)

    finish_nodes(node, pv, hot_sum, edge_low, v1[0, D:, :], v2[...], ngain[0:1, :], noff[0:1, :], keep)
    exchange(1)
    tables(1)
    for i in range(NBIG):
        r = strip(i, BIG)
        pre[r, :] = 0.5 * (dot(edge_low[r, :], w1[1, :D, :]) + eb1[1:2, :]) + dot(hot_local[r, :], table[...])
        state[r, :] += jnp.where(usable_rows(counts, i), eoff[1:2, :], 0.0)
    wait_sends(0)
    for c in range(3):
        halo_part(1, c)
    wait_part(1, 3)
    last_rows[...] = part_rows(1, 3)
    wait_sends(1)


def second_kernel(
    pre,
    state,
    node,
    pv,
    last_rows,
    hot_last,
    hot_sum,
    w2,
    v1,
    v2,
    counts,
    egain,
    ngain,
    noff,
    edge_out,
    node_out,
    result,
    nodes,
    hidden,
    product,
    low,
    edge_sem,
    node_sem,
):
    copies = []

    def put(i):
        r = pl.ds(i * BLK, BLK)
        copies.append(pltpu.make_async_copy(result.at[r], edge_out.at[r], edge_sem.at[i]))
        copies[-1].start()

    def put_nodes(i, value):
        nodes[strip(i, ROWS // 2), :] = value
        r = pl.ds(i * (ROWS // 2), ROWS // 2)
        copies.append(pltpu.make_async_copy(nodes.at[r], node_out.at[r], node_sem.at[i]))
        copies[-1].start()

    finish_edges(
        pre,
        state,
        hot_last,
        last_rows[...],
        counts,
        w2[...],
        egain[1:2, :],
        hidden,
        product,
        low,
        result,
        put,
    )
    finish_nodes(node, pv, hot_sum, low, v1[...], v2[...], ngain[1:2, :], noff[1:2, :], put_nodes)
    for c in copies:
        c.wait()


VMEM = pl.BlockSpec(memory_space=pltpu.VMEM)
SMEM = pl.BlockSpec(memory_space=pltpu.SMEM)
ANY = pl.BlockSpec(memory_space=pl.ANY)
HBM = pl.BlockSpec(memory_space=pltpu.HBM)


def shards(
    latents,
    edge_latents,
    edge_sender,
    edge_receiver,
    block_counts,
    send_rows,
    edge_first_weight,
    edge_first_bias,
    edge_second_weight,
    edge_gain,
    edge_offset,
    node_first_weight,
    node_first_bias,
    node_second_weight,
    node_gain,
    node_offset,
):
    snd = edge_sender.reshape(EDGE // 128, 128)
    rcv = edge_receiver.reshape(EDGE // 128, 128)
    lists = jnp.transpose(send_rows[0])
    shape = jax.ShapeDtypeStruct
    held = pl.pallas_call(
        first_kernel,
        out_shape=(
            pltpu.VMEM((EDGE, D), F32),
            pltpu.VMEM((EDGE, D), F32),
            pltpu.VMEM((ROWS, D), F32),
            pltpu.VMEM((ROWS, D), F32),
            pltpu.VMEM((256, D), BF16),
            pltpu.VMEM((EDGE, 256), BF16),
            pltpu.VMEM((ROWS, EDGE), BF16),
            pltpu.VMEM((D, D), BF16),
            pltpu.VMEM((D, D), BF16),
            pltpu.VMEM((D, D), BF16),
        ),
        in_specs=[HBM] * 16,
        out_specs=(VMEM,) * 10,
        scratch_shapes=[
            pltpu.VMEM((EDGE // 128, 128), jnp.int32),
            pltpu.VMEM((EDGE // 128, 128), jnp.int32),
            pltpu.SMEM((EDGE // 128,), jnp.int32),
            pltpu.VMEM((8, 128), jnp.int32),
            pltpu.VMEM((EDGE // 128, 128), F32),
        ]
        + [pltpu.VMEM((2, D), F32)] * 6
        + [
            pltpu.VMEM((2 * ROWS, HALF), F32),
            pltpu.VMEM((3, EDGE, 256), BF16),
            pltpu.VMEM((EDGE, 2 * ROWS), BF16),
            pltpu.VMEM((1024, ROWS), BF16),
            pltpu.VMEM((2, 3 * D, D), BF16),
            pltpu.VMEM((D, D), BF16),
            pltpu.VMEM((2, 2 * D, D), BF16),
            pltpu.VMEM((D, D), BF16),
            pltpu.VMEM((ROWS, HALF), BF16),
            pltpu.VMEM((ROWS, HALF), BF16),
            pltpu.VMEM((ROWS, D), BF16),
            pltpu.VMEM((EDGE, D), BF16),
            pltpu.VMEM((2, BLK, D), F32),
            pltpu.VMEM((EDGE, D), BF16),
            pltpu.VMEM((2 * ROWS, D), BF16),
            pltpu.VMEM((2, 128, 8, D), BF16),
            pltpu.VMEM((2, 128, 8, D), BF16),
            pltpu.SemaphoreType.DMA,
            pltpu.SemaphoreType.DMA((3,)),
            pltpu.SemaphoreType.DMA((NBIG,)),
            pltpu.SemaphoreType.DMA((16,)),
            pltpu.SemaphoreType.DMA((2,)),
            pltpu.SemaphoreType.DMA((2,)),
            pltpu.SemaphoreType.DMA((2,)),
            pltpu.SemaphoreType.DMA((2, 4)),
            pltpu.SemaphoreType.REGULAR,
        ],
        compiler_params=pltpu.CompilerParams(
            collective_id=0, has_side_effects=True, vmem_limit_bytes=47 * 1024 * 1024
        ),
    )(
        latents,
        edge_latents,
        snd,
        rcv,
        block_counts,
        lists,
        edge_first_weight,
        edge_first_bias,
        edge_second_weight,
        edge_gain,
        edge_offset,
        node_first_weight,
        node_first_bias,
        node_second_weight,
        node_gain,
        node_offset,
    )
    new_edges, new_nodes = pl.pallas_call(
        second_kernel,
        out_shape=(shape((EDGE, D), F32), shape((ROWS, D), F32)),
        in_specs=[VMEM] * 10 + [SMEM] + [VMEM] * 3,
        out_specs=(ANY, ANY),
        scratch_shapes=[
            pltpu.VMEM((EDGE, D), F32),
            pltpu.VMEM((ROWS, D), F32),
            pltpu.VMEM((EDGE, D), BF16),
            pltpu.VMEM((2, BLK, D), F32),
            pltpu.VMEM((EDGE, D), BF16),
            pltpu.SemaphoreType.DMA((EDGE // BLK,)),
            pltpu.SemaphoreType.DMA((2,)),
        ],
        compiler_params=pltpu.CompilerParams(vmem_limit_bytes=24 * 1024 * 1024),
    )(
        *held,
        block_counts,
        edge_gain,
        node_gain,
        node_offset,
    )
    return new_nodes, new_edges


def solution(mesh):
    split = P(("patch", "band"))
    return jax.shard_map(
        shards,
        mesh=mesh,
        in_specs=(
            P("patch", "band"),
            P(("patch", "band"), None),
            split,
            split,
            split,
            P(("patch", "band"), None, None),
        )
        + (P(),) * 10,
        out_specs=(P(("patch", "band"), None), P(("patch", "band"), None)),
        check_vma=False,
    )
```

```python
import functools

import jax
import jax.numpy as jnp
from jax import lax
from jax.experimental import pallas as pl
from jax.experimental.pallas import tpu as pltpu
from jax.sharding import PartitionSpec as P

MESH = pl.DeviceIdType.MESH
F32 = jnp.float32
BF16 = jnp.bfloat16
D = 512
HALF = 256
ROWS = 320
EDGE = 2560
BIG = 512
NBIG = EDGE // BIG
BLK = 256
PART = 32
EPS = 1e-05
STEP = 59
UNSTEP = 115


def dot(a, b):
    return jnp.dot(a, b, preferred_element_type=F32)


def swish(v):
    half = 0.5 * v
    return half + half * jnp.tanh(half)


def norm(v, gain, offset):
    centre = v - jnp.sum(v, axis=-1, keepdims=True) * (1.0 / D)
    spread = jnp.sum(centre * centre, axis=-1, keepdims=True) * (1.0 / D)
    return centre * lax.rsqrt(spread + EPS) * gain + offset


def column(row):
    return jnp.transpose(jnp.broadcast_to(row, (128, 128)))


def hot(match):
    return jnp.where(match, 1.0, 0.0).astype(BF16)


def lanes(base):
    return (lax.broadcasted_iota(jnp.int32, (128, 128), 1) + base).astype(F32)


def strip(i, size):
    return slice(i * size, (i + 1) * size)


def usable_rows(counts, block):
    row = lax.broadcasted_iota(jnp.int32, (128, 1), 0)
    n = BIG // 128
    return jnp.concatenate([row < counts[block * n + j] for j in range(n)], axis=0)


def finish_edges(pre, state, hot_last, rows, counts, w2, gain, hidden, product, low, out, done):
    for i in range(NBIG):
        r = strip(i, BIG)
        half = pre[r, :] + dot(hot_last[r, :], rows)
        hidden[r, :] = (half + half * jnp.tanh(half)).astype(BF16)
    row = lax.broadcasted_iota(jnp.int32, (PART, 1), 0)
    for i in range(EDGE // BLK):
        product[i % 2] = dot(hidden[strip(i, BLK), :], w2)
        for j in range(BLK // PART):
            first = i * BLK + j * PART
            r = slice(first, first + PART)
            value = product[i % 2, strip(j, PART), :]
            centre = value - jnp.sum(value, axis=-1, keepdims=True) * (1.0 / D)
            spread = jnp.sum(centre * centre, axis=-1, keepdims=True) * (1.0 / D)
            scale = jnp.where(row + first % 128 < counts[first // 128], lax.rsqrt(spread + EPS), 0.0)
            value = state[r, :] + centre * scale * gain
            out[r, :] = value
            low[r, :] = value.astype(BF16)
        done(i)


def finish_nodes(node, pv, hot_sum, edge_low, v1, w2, gain, offset, done):
    parts = [strip(i, ROWS // 2) for i in range(2)]
    sums = [dot(hot_sum[r, :], edge_low[...]).astype(BF16) for r in parts]
    hidden = [swish(pv[r, :] + dot(v, v1)).astype(BF16) for r, v in zip(parts, sums)]
    results = [dot(h, w2) for h in hidden]
    for i in range(2):
        done(i, node[parts[i], :] + norm(results[i], gain, offset))


def place():
    p = lax.axis_index("patch")
    b = lax.axis_index("band")
    core = p % 2
    z = (p // 2) % 4
    x = ((p // 8) % 2) * 2 + b
    y = p // 16
    return p, b, core, x, y, z


def at(core, x, y, z):
    return ((y * 2 + x // 2) * 4 + z) * 2 + core, x % 2


def apart(step):
    return step % 2, step // 2 % 4, step // 8 % 4, step // 32


def together(dc, dx, dy, dz):
    return dc % 2 + dx % 4 * 2 + dz % 4 * 8 + dy % 4 * 32


def distance(k):
    return sum(min(d, 4 - d) for d in apart(k * STEP % 128)[1:])


def number(core, x, y, z):
    patch, band = at(core % 2, x % 4, y % 4, z % 4)
    return patch * 2 + band


def first_kernel(
    latents,
    edges,
    snd_hbm,
    rcv_hbm,
    counts_hbm,
    lists_hbm,
    we1,
    eb1_hbm,
    we2,
    egain_hbm,
    eoff_hbm,
    wn1,
    nb1_hbm,
    wn2,
    ngain_hbm,
    noff_hbm,
    pre,
    state,
    node,
    pv,
    last_rows,
    hot_last,
    hot_sum,
    w2_next,
    v1_next,
    v2_next,
    snd,
    rcv,
    counts,
    lists,
    from_slot,
    eb1,
    egain,
    eoff,
    nb1,
    ngain,
    noff,
    lat,
    hot_halo,
    hot_local,
    hot_send,
    w1,
    w2,
    v1,
    v2,
    band_out,
    band_in,
    low,
    hidden,
    product,
    edge_low,
    table,
    stage,
    recv,
    list_sem,
    lat_sem,
    edge_sem,
    w_sem,
    band_send,
    band_recv,
    halo_send,
    halo_recv,
    greet,
):
    p, b, core, x, y, z = place()
    me = p * 2 + b
    barrier = pltpu.get_barrier_semaphore()
    plane = [(0, 0, dy, dz) for dy in range(4) for dz in range(4) if (dy, dz) != (0, 0)]
    line = [(dc, dx, 0, 0) for dc in range(2) for dx in range(4) if (dc, dx) != (0, 0)]

    def peer(dc, dx, dy, dz):
        return at((core + dc) % 2, (x + dx) % 4, (y + dy) % 4, (z + dz) % 4)

    half_rows = ROWS // 2
    lat_copies = []
    for i, d in enumerate((1 - b, 1 - b, b)):
        r = pl.ds(d * ROWS + (i % 2) * half_rows, half_rows) if i < 2 else pl.ds(d * ROWS, ROWS)
        lat_copies.append(pltpu.make_async_copy(latents.at[r], lat.at[r], lat_sem.at[i]))
        lat_copies[-1].start()
    list_copy = pltpu.make_async_copy(lists_hbm, lists, list_sem)
    list_copy.start()
    for o in line + plane:
        pl.semaphore_signal(barrier, inc=1, device_id=peer(*o), device_id_type=MESH)
    w_copies = [
        pltpu.make_async_copy(source, target, w_sem.at[i])
        for i, (source, target) in enumerate(
            (
                (we1, w1),
                (snd_hbm, snd),
                (rcv_hbm, rcv),
                (counts_hbm, counts),
                (eb1_hbm, eb1),
                (wn1, v1),
                (nb1_hbm, nb1),
                (we2.at[0], w2),
                (egain_hbm, egain),
                (eoff_hbm, eoff),
                (wn2.at[0], v2),
                (ngain_hbm, ngain),
                (noff_hbm, noff),
                (we2.at[1], w2_next),
                (wn1.at[1, pl.ds(D, D)], v1_next),
                (wn2.at[1], v2_next),
            )
        )
    ]
    edge_copies = [
        pltpu.make_async_copy(edges.at[pl.ds(i * BIG, BIG)], state.at[pl.ds(i * BIG, BIG)], edge_sem.at[i])
        for i in range(NBIG)
    ]

    for i in range(2):
        lat_copies[i].wait()
        band_out[strip(i, half_rows), :] = lat[pl.ds((1 - b) * ROWS + i * half_rows, half_rows), :].astype(BF16)
    for c in w_copies[:5] + edge_copies + w_copies[5:]:
        c.start()

    pl.semaphore_wait(barrier, len(plane) + len(line))
    for o in line:
        pl.semaphore_signal(greet, inc=1, device_id=peer(*o), device_id_type=MESH)
    band_copies = []
    for i in range(2):
        r = pl.ds(i * half_rows, half_rows)
        copy = pltpu.make_async_remote_copy(
            src_ref=band_out.at[r],
            dst_ref=band_in.at[r],
            send_sem=band_send.at[i],
            recv_sem=band_recv.at[i],
            device_id=(p, 1 - b),
            device_id_type=MESH,
        )
        copy.start()
        band_copies.append(copy)

    list_copy.wait()
    step = lax.broadcasted_iota(jnp.int32, (1, 128), 1) * STEP % 128
    dc, dx, dz, dy = apart(step)
    asks = (lax.broadcasted_iota(jnp.int32, (128, 128), 0) == number(core + dc, x + dx, y + dy, z + dz)).astype(F32)
    asks = asks.astype(BF16)
    high = lists[...] // 256
    low_part = dot((lists[...] - 256 * high).astype(F32).astype(BF16), asks)
    wanted = 256.0 * dot(high.astype(F32).astype(BF16), asks) + low_part
    for c in range(8):
        block = jnp.concatenate(
            [jnp.broadcast_to(wanted[:, q : q + 1], (8, 128)) for q in range(16 * c, 16 * c + 16)], axis=0
        )
        for t in range(3):
            wide = 128 if t < 2 else 64
            hot_send[strip(c, 128), t * 128 : t * 128 + wide] = hot(block == lanes(t * 128))[:, :wide]

    def project(layer, i):
        r = strip(i, half_rows)
        low[r, :] = node[r, :].astype(BF16)
        table[r, :] = (0.5 * dot(low[r, :], w1[layer, D : 2 * D, :])).astype(BF16)

    w_copies[0].wait()
    lat_copies[2].wait()
    for i in range(2):
        band_copies[i].wait()
        r = strip(i, half_rows)
        own = lat[pl.ds(b * ROWS + i * half_rows, half_rows), :]
        other = band_in[r, :].astype(F32)
        node[r, :HALF] = jnp.where(b == 0, own, other)
        node[r, HALF:] = jnp.where(b == 0, other, own)
        project(0, i)

    xs = [(x + d) % 4 for d in range(4)]

    def exchange(layer):
        def fill(first, last):
            chosen = dot(hot_send[first * 8 : last * 8, :], table[:ROWS, :]).astype(BF16)
            stage[layer, first:last] = chosen.reshape(last - first, 8, D)

        def send(first, last):
            for k in sorted(range(max(first, 1), last), key=lambda k: -distance(k)):
                dc, dx, dz, dy = apart(k * STEP % 128)
                px = (y + dy) % 4 * 16 + xs[dx] // 2 * 8 + (z + dz) % 4 * 2 + (core + dc) % 2
                pltpu.make_async_remote_copy(
                    src_ref=stage.at[layer, k],
                    dst_ref=recv.at[layer, k],
                    send_sem=halo_send.at[layer],
                    recv_sem=halo_recv.at[layer, k // 32],
                    device_id=(px, xs[dx] % 2),
                    device_id_type=MESH,
                ).start()

        cuts = (0, 16, 32, 64, 96, 128)
        fill(0, 16)
        if layer == 0:
            pl.semaphore_wait(greet, len(line))
        for i in range(1, 6):
            if i < 5:
                fill(cuts[i], cuts[i + 1])
            send(cuts[i - 1], cuts[i])
        recv[layer, 0] = stage[layer, 0]

    def tables(layer):
        table[ROWS:, :] = (0.5 * dot(low[...], w1[layer, 2 * D :, :])).astype(BF16)
        pv[...] = dot(low[...], v1[layer, :D, :]) + nb1[layer : layer + 1, :]

    def wait_part(layer, c):
        n = 31 if c == 0 else 32
        pltpu.make_async_copy(
            stage.at[layer, pl.ds(0, n)], recv.at[layer, pl.ds(0, n)], halo_recv.at[layer, c]
        ).wait()

    def part_rows(layer, c):
        return recv[layer, strip(c, 32)].reshape(256, D)

    def halo_part(layer, c):
        wait_part(layer, c)
        for i in range(NBIG):
            r = strip(i, BIG)
            pre[r, :] += dot(hot_halo[c, r, :], part_rows(layer, c))

    def wait_sends(layer):
        pltpu.make_async_copy(
            stage.at[layer, pl.ds(0, 127)], recv.at[layer, pl.ds(0, 127)], halo_send.at[layer]
        ).wait()

    exchange(0)
    for c in w_copies[1:5]:
        c.wait()

    remote = snd[...] - ROWS
    dev = remote // 8
    step = together(
        core - dev // 2 % 2 + 2,
        x - (dev // 16 % 2 * 2 + dev % 2) + 4,
        y - dev // 32 + 4,
        z - dev // 4 % 4 + 4,
    )
    place_of = ROWS + step * UNSTEP % 128 * 8 + remote % 8
    from_slot[...] = jnp.where(remote < 0, snd[...], place_of).astype(F32)

    def hots(i, _):
        rows = pl.ds(pl.multiple_of(i * 128, 128), 128)
        s = column(from_slot[pl.ds(i, 1), :])
        r = column(rcv[pl.ds(i, 1), :].astype(F32)) + float(ROWS)
        lane = lax.broadcasted_iota(jnp.int32, (128, 128), 1)
        mixed = jnp.where(lane < 64, s, r)
        for t, source in enumerate((s, s, mixed, r, r)):
            hot_local[rows, t * 128 : t * 128 + 128] = hot(source == lanes(t * 128))
        for t in range(8):
            part = hot(s == lanes(ROWS + t * 128))
            if t < 6:
                hot_halo[t // 2, rows, t % 2 * 128 : t % 2 * 128 + 128] = part
            else:
                hot_last[rows, t % 2 * 128 : t % 2 * 128 + 128] = part
        target = jnp.where(lane[:1] < counts[i], rcv[pl.ds(i, 1), :], -1)
        hot_sum[:, rows] = hot(lax.broadcasted_iota(jnp.int32, (ROWS, 128), 0) == target)
        return 0

    lax.fori_loop(0, EDGE // 128, hots, 0)
    for c in edge_copies + w_copies[5:]:
        c.wait()
    tables(0)
    for i in range(NBIG):
        r = strip(i, BIG)
        edge_part = 0.5 * (dot(state[r, :].astype(BF16), w1[0, :D, :]) + eb1[0:1, :])
        pre[r, :] = edge_part + dot(hot_local[r, :], table[...])
        state[r, :] += jnp.where(usable_rows(counts, i), eoff[0:1, :], 0.0)
    for c in range(3):
        halo_part(0, c)
    wait_part(0, 3)

    finish_edges(
        pre,
        state,
        hot_last,
        part_rows(0, 3),
        counts,
        w2[...],
        egain[0:1, :],
        hidden,
        product,
        edge_low,
        state,
        lambda i: None,
    )

    def keep(i, value):
        node[strip(i, ROWS // 2), :] = value
        project(1, i)

    finish_nodes(node, pv, hot_sum, edge_low, v1[0, D:, :], v2[...], ngain[0:1, :], noff[0:1, :], keep)
    exchange(1)
    tables(1)
    for i in range(NBIG):
        r = strip(i, BIG)
        pre[r, :] = 0.5 * (dot(edge_low[r, :], w1[1, :D, :]) + eb1[1:2, :]) + dot(hot_local[r, :], table[...])
        state[r, :] += jnp.where(usable_rows(counts, i), eoff[1:2, :], 0.0)
    wait_sends(0)
    for c in range(3):
        halo_part(1, c)
    wait_part(1, 3)
    last_rows[...] = part_rows(1, 3)
    wait_sends(1)


def second_kernel(
    pre,
    state,
    node,
    pv,
    last_rows,
    hot_last,
    hot_sum,
    w2,
    v1,
    v2,
    counts,
    egain,
    ngain,
    noff,
    edge_out,
    node_out,
    result,
    nodes,
    hidden,
    product,
    low,
    edge_sem,
    node_sem,
):
    copies = []

    def put(i):
        r = pl.ds(i * BLK, BLK)
        copies.append(pltpu.make_async_copy(result.at[r], edge_out.at[r], edge_sem.at[i]))
        copies[-1].start()

    def put_nodes(i, value):
        nodes[strip(i, ROWS // 2), :] = value
        r = pl.ds(i * (ROWS // 2), ROWS // 2)
        copies.append(pltpu.make_async_copy(nodes.at[r], node_out.at[r], node_sem.at[i]))
        copies[-1].start()

    finish_edges(
        pre,
        state,
        hot_last,
        last_rows[...],
        counts,
        w2[...],
        egain[1:2, :],
        hidden,
        product,
        low,
        result,
        put,
    )
    finish_nodes(node, pv, hot_sum, low, v1[...], v2[...], ngain[1:2, :], noff[1:2, :], put_nodes)
    for c in copies:
        c.wait()


VMEM = pl.BlockSpec(memory_space=pltpu.VMEM)
SMEM = pl.BlockSpec(memory_space=pltpu.SMEM)
ANY = pl.BlockSpec(memory_space=pl.ANY)
HBM = pl.BlockSpec(memory_space=pltpu.HBM)


def shards(
    latents,
    edge_latents,
    edge_sender,
    edge_receiver,
    block_counts,
    send_rows,
    edge_first_weight,
    edge_first_bias,
    edge_second_weight,
    edge_gain,
    edge_offset,
    node_first_weight,
    node_first_bias,
    node_second_weight,
    node_gain,
    node_offset,
):
    snd = edge_sender.reshape(EDGE // 128, 128)
    rcv = edge_receiver.reshape(EDGE // 128, 128)
    lists = jnp.transpose(send_rows[0])
    shape = jax.ShapeDtypeStruct
    held = pl.pallas_call(
        first_kernel,
        out_shape=(
            pltpu.VMEM((EDGE, D), F32),
            pltpu.VMEM((EDGE, D), F32),
            pltpu.VMEM((ROWS, D), F32),
            pltpu.VMEM((ROWS, D), F32),
            pltpu.VMEM((256, D), BF16),
            pltpu.VMEM((EDGE, 256), BF16),
            pltpu.VMEM((ROWS, EDGE), BF16),
            pltpu.VMEM((D, D), BF16),
            pltpu.VMEM((D, D), BF16),
            pltpu.VMEM((D, D), BF16),
        ),
        in_specs=[HBM] * 16,
        out_specs=(VMEM,) * 10,
        scratch_shapes=[
            pltpu.VMEM((EDGE // 128, 128), jnp.int32),
            pltpu.VMEM((EDGE // 128, 128), jnp.int32),
            pltpu.SMEM((EDGE // 128,), jnp.int32),
            pltpu.VMEM((8, 128), jnp.int32),
            pltpu.VMEM((EDGE // 128, 128), F32),
        ]
        + [pltpu.VMEM((2, D), F32)] * 6
        + [
            pltpu.VMEM((2 * ROWS, HALF), F32),
            pltpu.VMEM((3, EDGE, 256), BF16),
            pltpu.VMEM((EDGE, 2 * ROWS), BF16),
            pltpu.VMEM((1024, ROWS), BF16),
            pltpu.VMEM((2, 3 * D, D), BF16),
            pltpu.VMEM((D, D), BF16),
            pltpu.VMEM((2, 2 * D, D), BF16),
            pltpu.VMEM((D, D), BF16),
            pltpu.VMEM((ROWS, HALF), BF16),
            pltpu.VMEM((ROWS, HALF), BF16),
            pltpu.VMEM((ROWS, D), BF16),
            pltpu.VMEM((EDGE, D), BF16),
            pltpu.VMEM((2, BLK, D), F32),
            pltpu.VMEM((EDGE, D), BF16),
            pltpu.VMEM((2 * ROWS, D), BF16),
            pltpu.VMEM((2, 128, 8, D), BF16),
            pltpu.VMEM((2, 128, 8, D), BF16),
            pltpu.SemaphoreType.DMA,
            pltpu.SemaphoreType.DMA((3,)),
            pltpu.SemaphoreType.DMA((NBIG,)),
            pltpu.SemaphoreType.DMA((16,)),
            pltpu.SemaphoreType.DMA((2,)),
            pltpu.SemaphoreType.DMA((2,)),
            pltpu.SemaphoreType.DMA((2,)),
            pltpu.SemaphoreType.DMA((2, 4)),
            pltpu.SemaphoreType.REGULAR,
        ],
        compiler_params=pltpu.CompilerParams(
            collective_id=0, has_side_effects=True, vmem_limit_bytes=47 * 1024 * 1024
        ),
    )(
        latents,
        edge_latents,
        snd,
        rcv,
        block_counts,
        lists,
        edge_first_weight,
        edge_first_bias,
        edge_second_weight,
        edge_gain,
        edge_offset,
        node_first_weight,
        node_first_bias,
        node_second_weight,
        node_gain,
        node_offset,
    )
    new_edges, new_nodes = pl.pallas_call(
        second_kernel,
        out_shape=(shape((EDGE, D), F32), shape((ROWS, D), F32)),
        in_specs=[VMEM] * 10 + [SMEM] + [VMEM] * 3,
        out_specs=(ANY, ANY),
        scratch_shapes=[
            pltpu.VMEM((EDGE, D), F32),
            pltpu.VMEM((ROWS, D), F32),
            pltpu.VMEM((EDGE, D), BF16),
            pltpu.VMEM((2, BLK, D), F32),
            pltpu.VMEM((EDGE, D), BF16),
            pltpu.SemaphoreType.DMA((EDGE // BLK,)),
            pltpu.SemaphoreType.DMA((2,)),
        ],
        compiler_params=pltpu.CompilerParams(vmem_limit_bytes=24 * 1024 * 1024),
    )(
        *held,
        block_counts,
        edge_gain,
        node_gain,
        node_offset,
    )
    return new_nodes, new_edges


def solution(mesh):
    split = P(("patch", "band"))
    return jax.shard_map(
        shards,
        mesh=mesh,
        in_specs=(
            P("patch", "band"),
            P(("patch", "band"), None),
            split,
            split,
            split,
            P(("patch", "band"), None, None),
        )
        + (P(),) * 10,
        out_specs=(P(("patch", "band"), None), P(("patch", "band"), None)),
        check_vma=False,
    )
```
